32 devices in a mesh: vp: 4 (over z), dp: 8 (over y, x, core).
Axes of the slice: x: 2, y: 2, z: 4, core: 2. Of those that a mesh axis runs over, the one named last changes fastest.
Arguments:
- h_last: bfloat16 [4096, 49, 1024], P('dp')
- ln_gamma: float32 [1024], replicated
- ln_beta: float32 [1024], replicated
- w_cls: bfloat16 [1024, 22016], P(None, 'vp')
- b_cls: float32 [22016], P('vp')
- targets: float32 [4096, 22016], P('dp', 'vp')
Outputs:
- output 1: float32 [], replicated
- output 2: float32 [1024, 22016], P(None, 'vp')
- output 3: float32 [22016], P('vp')
- output 4: bfloat16 [4096, 49, 1024], P('dp')
All inputs are finite; a program needn't handle non-finite values.
Results may differ from the reference program's by a relative error of at most 0.001.
Values sent between devices are 32-bit elements.
A program may use at most 1 GiB of HBM per device.

```python
import jax
import jax.numpy as jnp
from jax import lax

IMG_DEV = 512
DP_SIZE = 8
TOKENS = 49
WIDTH = 1024
CLASSES = 21841
CLASSES_PAD = 22016
N_GLOB = IMG_DEV * DP_SIZE
LN_EPS = 1e-5


def pool_norm(h_blk, ln_gamma, ln_beta):
    h_wide = h_blk.astype(jnp.float32)
    tok_mean = h_wide.mean(axis=-1, keepdims=True)
    centered = h_wide - tok_mean
    tok_var = (centered * centered).mean(axis=-1, keepdims=True)
    normed = centered * lax.rsqrt(tok_var + LN_EPS)
    return (normed * ln_gamma + ln_beta).mean(axis=1)


def setup_inputs(seed: int = 0) -> dict:
    root_key = jax.random.key(seed)
    sub_keys = jax.random.split(root_key, 8)
    img_base = jax.random.normal(sub_keys[0], (N_GLOB, 1, WIDTH), jnp.float32)
    tok_noise = jax.random.normal(sub_keys[1], (N_GLOB, TOKENS, WIDTH), jnp.float32)
    h_last = (img_base + 0.5 * tok_noise).astype(jnp.bfloat16)
    ln_gamma = 2.0 + 0.5 * jax.random.normal(sub_keys[2], (WIDTH,), jnp.float32)
    ln_beta = 0.5 * jax.random.normal(sub_keys[3], (WIDTH,), jnp.float32)
    w_cls = (jax.random.normal(sub_keys[4], (WIDTH, CLASSES_PAD), jnp.float32) * WIDTH ** -0.5).astype(jnp.bfloat16)
    b_cls = jax.random.normal(sub_keys[5], (CLASSES_PAD,), jnp.float32)
    classes = jax.random.randint(sub_keys[6], (N_GLOB, 2), 0, CLASSES)
    mix_lam = jax.random.uniform(sub_keys[7], (N_GLOB, 1), jnp.float32)
    col_idx = jnp.arange(CLASSES_PAD)
    first_hit = (col_idx[None, :] == classes[:, 0:1]).astype(jnp.float32)
    second_hit = (col_idx[None, :] == classes[:, 1:2]).astype(jnp.float32)
    smooth = jnp.where(col_idx < CLASSES, 0.1 / CLASSES, 0.0)
    targets = 0.9 * (mix_lam * first_hit + (1.0 - mix_lam) * second_hit) + smooth[None, :]
    return {"h_last": h_last, "ln_gamma": ln_gamma, "ln_beta": ln_beta, "w_cls": w_cls, "b_cls": b_cls, "targets": targets}


def reference(h_last, ln_gamma, ln_beta, w_cls, b_cls, targets):
    in_range = jnp.arange(CLASSES_PAD) < CLASSES
    h_blocks = h_last.reshape(DP_SIZE, IMG_DEV, TOKENS, WIDTH)
    t_blocks = targets.reshape(DP_SIZE, IMG_DEV, CLASSES_PAD)

    def block_step(acc_state, block_in):
        dw_acc, db_acc, loss_acc = acc_state
        h_blk, t_blk = block_in
        pooled, pool_vjp = jax.vjp(lambda h_in: pool_norm(h_in, ln_gamma, ln_beta), h_blk)
        pooled_bf = pooled.astype(jnp.bfloat16)
        logits = jnp.dot(pooled_bf, w_cls, preferred_element_type=jnp.float32) + b_cls
        masked = jnp.where(in_range, logits, -jnp.inf)
        log_norm = jax.nn.logsumexp(masked, axis=1)
        t_sum = t_blk.sum(axis=1)
        t_dot = (t_blk * jnp.where(in_range, logits, 0.0)).sum(axis=1)
        soft_prob = jnp.exp(masked - log_norm[:, None])
        dlogits = (soft_prob * t_sum[:, None] - t_blk) / N_GLOB
        dlog_bf = dlogits.astype(jnp.bfloat16)
        dw_blk = jnp.dot(pooled_bf.T, dlog_bf, preferred_element_type=jnp.float32)
        d_pooled = jnp.dot(dlog_bf, w_cls.T, preferred_element_type=jnp.float32)
        dh_blk = pool_vjp(d_pooled)[0]
        loss_blk = (log_norm * t_sum - t_dot).sum()
        return (dw_acc + dw_blk, db_acc + dlogits.sum(axis=0), loss_acc + loss_blk), dh_blk

    carry_init = (jnp.zeros((WIDTH, CLASSES_PAD), jnp.float32), jnp.zeros((CLASSES_PAD,), jnp.float32), jnp.zeros((), jnp.float32))
    (dw_cls, db_cls, loss_sum), dh_blocks = lax.scan(block_step, carry_init, (h_blocks, t_blocks))
    return loss_sum / N_GLOB, dw_cls, db_cls, dh_blocks.reshape(N_GLOB, TOKENS, WIDTH)
```

```python
import functools

import jax
import jax.numpy as jnp
from jax import lax
from jax.experimental import pallas as pl
from jax.experimental.pallas import tpu as pltpu
from jax.sharding import PartitionSpec as P

NUM_CLASSES = 21841
LN_EPS = 1e-5
F32 = jnp.float32
BF16 = jnp.bfloat16


def norm_rows(x):
    width = x.shape[-1]
    c = x - x.sum(axis=-1, keepdims=True) * (1.0 / width)
    var = (c * c).sum(axis=-1, keepdims=True) * (1.0 / width)
    return c, lax.rsqrt(var + LN_EPS)


def pool_kernel(h_ref, gamma_ref, beta_ref, u_ref, acc_ref):
    tokens, rows, _ = h_ref.shape

    acc_ref[...] = jnp.zeros_like(acc_ref)

    def group(i, carry):
        r0 = pl.multiple_of(i * 16, 16)

        def token(t, carry):
            c, r = norm_rows(h_ref[t, pl.ds(r0, 16), :].astype(F32))
            acc_ref[pl.ds(r0, 16), :] += c * r
            return carry

        return lax.fori_loop(0, tokens, token, carry, unroll=True)

    lax.fori_loop(0, rows // 16, group, 0)
    u = acc_ref[...] * (gamma_ref[...] * (1.0 / tokens)) + beta_ref[...]
    u_ref[...] = u.astype(BF16)


def pool_forward(ht, gamma, beta, rows=64):
    tokens, images, width = ht.shape
    rows = min(rows, images)
    return pl.pallas_call(
        pool_kernel,
        grid=(images // rows,),
        in_specs=[
            pl.BlockSpec((tokens, rows, width), lambda i: (0, i, 0)),
            pl.BlockSpec((1, width), lambda i: (0, 0)),
            pl.BlockSpec((1, width), lambda i: (0, 0)),
        ],
        out_specs=pl.BlockSpec((rows, width), lambda i: (i, 0)),
        out_shape=jax.ShapeDtypeStruct((images, width), BF16),
        scratch_shapes=[pltpu.VMEM((rows, width), F32)],
        compiler_params=pltpu.CompilerParams(dimension_semantics=("arbitrary",)),
        cost_estimate=pl.CostEstimate(flops=8 * ht.size * 40, bytes_accessed=2 * ht.size, transcendentals=0),
        name="pool_forward",
    )(ht, gamma[None], beta[None])


def pool_backward_kernel(h_ref, du_ref, gamma_ref, *rest):
    dh_ref, v_ref = rest[-2:]
    tokens, rows, width = h_ref.shape
    v = du_ref[...] * (gamma_ref[...] * (1.0 / tokens))
    v_ref[...] = v - v.sum(axis=-1, keepdims=True) * (1.0 / width)

    def group(i, carry):
        r0 = pl.multiple_of(i * 16, 16)

        def token(t, carry):
            c, r = norm_rows(h_ref[t, pl.ds(r0, 16), :].astype(F32))
            vc = v_ref[pl.ds(r0, 16), :]
            xhat = c * r
            k = (vc * xhat).sum(axis=-1, keepdims=True) * (1.0 / width)
            dh_ref[t, pl.ds(r0, 16), :] = ((vc - xhat * k) * r).astype(BF16)
            return carry

        return lax.fori_loop(0, tokens, token, carry, unroll=True)

    lax.fori_loop(0, rows // 16, group, 0)


def pool_backward(ht, du, gamma, buf, first, count, rows=64):
    tokens, images, width = ht.shape
    rows = min(rows, count)
    off = first // rows
    in_specs = [
        pl.BlockSpec((tokens, rows, width), lambda i: (0, i + off, 0)),
        pl.BlockSpec((rows, width), lambda i: (i + off, 0)),
        pl.BlockSpec((1, width), lambda i: (0, 0)),
    ]
    args = [ht, du, gamma[None]]
    aliases = {}
    if buf is not None:
        in_specs.append(pl.BlockSpec(memory_space=pl.ANY))
        args.append(buf)
        aliases = {3: 0}
    return pl.pallas_call(
        pool_backward_kernel,
        grid=(count // rows,),
        in_specs=in_specs,
        out_specs=pl.BlockSpec((tokens, rows, width), lambda i: (0, i + off, 0)),
        out_shape=jax.ShapeDtypeStruct((tokens, images, width), BF16),
        scratch_shapes=[pltpu.VMEM((rows, width), F32)],
        input_output_aliases=aliases,
        compiler_params=pltpu.CompilerParams(dimension_semantics=("arbitrary",)),
        cost_estimate=pl.CostEstimate(
            flops=40 * 12 * tokens * count * width, bytes_accessed=4 * tokens * count * width, transcendentals=0
        ),
        name="pool_backward",
    )(*args)


def logits_kernel(limit_ref, u_ref, w_ref, b_ref, t_ref, z_ref, stat_ref, m_ref, s_ref, ts_ref, tz_ref):
    step = pl.program_id(0)
    cols = w_ref.shape[1]

    @pl.when(step == 0)
    def _():
        m_ref[...] = jnp.full_like(m_ref, -jnp.inf)
        s_ref[...] = jnp.zeros_like(s_ref)
        ts_ref[...] = jnp.zeros_like(ts_ref)
        tz_ref[...] = jnp.zeros_like(tz_ref)

    z = jnp.dot(u_ref[...], w_ref[...], preferred_element_type=F32) + b_ref[...]
    col = step * cols + lax.broadcasted_iota(jnp.int32, (1, cols), 1)
    valid = col < limit_ref[0]
    t = jnp.where(valid, t_ref[...], 0.0)
    tz = t * jnp.where(valid, z, 0.0)
    z = jnp.where(valid, z, -jnp.inf)
    z_ref[...] = z
    parts = [slice(k, k + 128) for k in range(0, cols, 128)]
    m_old = m_ref[...]
    m_new = m_old
    for p in parts:
        m_new = jnp.maximum(m_new, z[:, p])
    base = jnp.where(m_new == -jnp.inf, 0.0, m_new)
    s = s_ref[...] * jnp.exp(m_old - base)
    ts = ts_ref[...]
    tzs = tz_ref[...]
    for p in parts:
        s += jnp.exp(z[:, p] - base)
        ts += t[:, p]
        tzs += tz[:, p]
    m_ref[...] = m_new
    s_ref[...] = s
    ts_ref[...] = ts
    tz_ref[...] = tzs

    @pl.when(step == pl.num_programs(0) - 1)
    def _():
        m = m_ref[...].max(axis=1, keepdims=True)
        s = (s_ref[...] * jnp.exp(m_ref[...] - m)).sum(axis=1, keepdims=True)
        ts = ts_ref[...].sum(axis=1, keepdims=True)
        tz = tz_ref[...].sum(axis=1, keepdims=True)
        lane = lax.broadcasted_iota(jnp.int32, m_ref.shape, 1)
        packed = jnp.where(lane == 0, m, jnp.where(lane == 1, s, jnp.where(lane == 2, ts, tz)))
        stat_ref[...] = packed.T[:8]


def logits_call(limit, u, w, b, t, cols=512):
    images, width = u.shape
    classes = w.shape[1]
    cols = min(cols, classes)
    lane_stat = pltpu.VMEM((images, 128), F32)
    return pl.pallas_call(
        logits_kernel,
        grid_spec=pltpu.PrefetchScalarGridSpec(
            num_scalar_prefetch=1,
            grid=(pl.cdiv(classes, cols),),
            in_specs=[
                pl.BlockSpec((images, width), lambda i, s: (0, 0)),
                pl.BlockSpec((width, cols), lambda i, s: (0, i)),
                pl.BlockSpec((1, cols), lambda i, s: (0, i)),
                pl.BlockSpec((images, cols), lambda i, s: (0, i)),
            ],
            out_specs=[
                pl.BlockSpec((images, cols), lambda i, s: (0, i)),
                pl.BlockSpec((8, images), lambda i, s: (0, 0)),
            ],
            scratch_shapes=[lane_stat] * 4,
        ),
        out_shape=[
            jax.ShapeDtypeStruct((images, classes), F32),
            jax.ShapeDtypeStruct((8, images), F32),
        ],
        compiler_params=pltpu.CompilerParams(dimension_semantics=("arbitrary",)),
        cost_estimate=pl.CostEstimate(
            flops=2 * images * width * classes, bytes_accessed=2 * width * classes, transcendentals=images * classes
        ),
        name="logits",
    )(limit, u, w, b[None], t)


def grad_kernel(n_glob, stat_ref, z_ref, t_ref, g_ref, db_ref, loss_ref, col_ref):
    shards = stat_ref.shape[0]

    @pl.when(pl.program_id(0) == 0)
    def _():
        stat = [stat_ref[k] for k in range(shards)]
        m = functools.reduce(jnp.maximum, [a[0:1] for a in stat])
        s = sum(a[1:2] * jnp.exp(a[0:1] - m) for a in stat)
        ts = sum(a[2:3] for a in stat)
        tz = sum(a[3:4] for a in stat)
        log_norm = m + jnp.log(s)
        loss_ref[...] = (log_norm * ts - tz).sum(axis=1, keepdims=True) + jnp.zeros_like(loss_ref)
        row = lax.broadcasted_iota(jnp.int32, (128, m.shape[1]), 0)
        col_ref[...] = jnp.where(row == 0, log_norm, ts).T

    log_norm = col_ref[:, 0:1]
    ts = col_ref[:, 1:2]
    g = (jnp.exp(z_ref[...] - log_norm) * ts - t_ref[...]) * (1.0 / n_glob)
    g_ref[...] = g.astype(BF16)
    db_ref[...] = g.sum(axis=0, keepdims=True)


def grad_call(stats, z, t, n_glob, cols=512):
    images, classes = z.shape
    cols = min(cols, classes)
    return pl.pallas_call(
        functools.partial(grad_kernel, n_glob),
        grid=(pl.cdiv(classes, cols),),
        in_specs=[
            pl.BlockSpec(stats.shape, lambda i: (0, 0, 0)),
            pl.BlockSpec((images, cols), lambda i: (0, i)),
            pl.BlockSpec((images, cols), lambda i: (0, i)),
        ],
        out_specs=[
            pl.BlockSpec((images, cols), lambda i: (0, i)),
            pl.BlockSpec((1, cols), lambda i: (0, i)),
            pl.BlockSpec((1, 128), lambda i: (0, 0)),
        ],
        out_shape=[
            jax.ShapeDtypeStruct((images, classes), BF16),
            jax.ShapeDtypeStruct((1, classes), F32),
            jax.ShapeDtypeStruct((1, 128), F32),
        ],
        scratch_shapes=[pltpu.VMEM((images, 128), F32)],
        compiler_params=pltpu.CompilerParams(dimension_semantics=("arbitrary",)),
        cost_estimate=pl.CostEstimate(flops=1000 * z.size, bytes_accessed=10 * z.size, transcendentals=z.size),
        name="grad",
    )(stats, z, t)


def solution(mesh):
    dp_size = mesh.shape["dp"]
    vp_size = mesh.shape["vp"]
    sibling = [(i, i ^ 1) for i in range(8)]
    first = [(i, i ^ (4 if i & 1 else 2)) for i in range(8)]
    second = [(i, i ^ (2 if i & 1 else 4)) for i in range(8)]

    def local_step(h_loc, gamma, beta, w_loc, b_loc, t_loc):
        images, _, width = h_loc.shape
        n_glob = images * dp_size
        classes = w_loc.shape[1]
        part = width // 8
        dp = lax.axis_index("dp")
        vp = lax.axis_index("vp")
        core, x, y = dp & 1, (dp >> 1) & 1, dp >> 2
        p1 = jnp.where(core == 0, x, y)
        p2 = jnp.where(core == 0, y, x)
        own = [4 * core + 2 * a + b for a, b in ((1 - p1, 1 - p2), (1 - p1, p2), (p1, 1 - p2), (p1, p2))]
        sib = [4 * (1 - core) + 2 * a + b for a, b in ((1 - p2, 1 - p1), (1 - p2, p1), (p2, 1 - p1), (p2, p1))]

        ht = h_loc.transpose(1, 0, 2)
        u = pool_forward(ht, gamma, beta)
        limit = jnp.minimum(classes, NUM_CLASSES - vp * classes).astype(jnp.int32)[None]
        z, stat = logits_call(limit, u, w_loc, b_loc, t_loc)
        stats = lax.all_gather(stat, "vp")
        g, db_part, loss_part = grad_call(stats, z, t_loc, n_glob)

        u_parts = jnp.concatenate(
            [lax.dynamic_slice(u, (0, k * part), (images, part)) for k in sib + own], axis=1
        )

        def dw(lo, hi):
            return lax.dot_general(
                u_parts[:, lo * part : hi * part], g, (((0,), (0,)), ((), ())), preferred_element_type=F32
            )

        def send(a, pairs):
            return lax.ppermute(a, "dp", pairs)

        s_a = send(dw(0, 1), sibling)
        s_b = send(dw(1, 2), sibling)
        a = dw(4, 5) + s_a
        r_c = send(a, first)
        b = dw(5, 6) + s_b
        r_d = send(b, first)
        s_cd = send(dw(2, 4), sibling)
        c_own = dw(6, 7)
        d_own = dw(7, 8)
        c = c_own + s_cd[:part] + r_c
        r_d2 = send(c, second)
        d = (d_own + s_cd[part:] + r_d) + r_d2
        c_fin = send(d, second)
        b_fin = send(d, first)
        a_fin = send(c_fin, first)
        mine = [a_fin, b_fin, c_fin, d]
        theirs = [send(v, sibling) for v in mine]

        du_part = lax.dot_general(g, w_loc, (((1,), (1,)), ((), ())), preferred_element_type=F32)
        z0, z1 = vp & 1, vp >> 1
        near = [(i, i ^ 1) for i in range(vp_size)]
        far = [(i, i ^ 2) for i in range(vp_size)]
        half, quarter = images // 2, images // 4

        def rows(v, k, n):
            return lax.dynamic_slice(v, (k * n, 0), (n, width))

        got = lax.ppermute(rows(du_part, 1 - z0, half), "vp", near)
        du_half = rows(du_part, z0, half) + got
        got = lax.ppermute(rows(du_half, 1 - z1, quarter), "vp", far)
        du_quarter = rows(du_half, z1, quarter) + got
        got = lax.ppermute(du_quarter, "vp", far)
        low = jnp.where(z1 == 0, du_quarter, got)
        high = jnp.where(z1 == 0, got, du_quarter)
        du_half = jnp.concatenate([low, high], axis=0)
        got = lax.ppermute(du_half, "vp", near)
        low = jnp.where(z0 == 0, du_half, got)
        high = jnp.where(z0 == 0, got, du_half)
        du = jnp.concatenate([low, high], axis=0)

        dh = None
        for k in range(4):
            dh = pool_backward(ht, du, gamma, dh, k * quarter, quarter)

        db_part, loss_part, _ = lax.optimization_barrier((db_part, loss_part, a))
        db_sum, loss_sum = lax.psum((db_part, loss_part), "dp")

        out = jnp.zeros((width, classes), F32)
        for v, k in ((mine[3], own[3]), (theirs[3], sib[3]), (mine[2], own[2]), (theirs[2], sib[2]),
                     (mine[1], own[1]), (theirs[1], sib[1]), (mine[0], own[0]), (theirs[0], sib[0])):
            out = lax.dynamic_update_slice(out, v, (k * part, 0))
        return loss_sum[0, 0] / n_glob, out, db_sum[0], dh.transpose(1, 0, 2)

    return jax.shard_map(
        local_step,
        mesh=mesh,
        in_specs=(P("dp", None, None), P(), P(), P(None, "vp"), P("vp"), P("dp", "vp")),
        out_specs=(P(), P(None, "vp"), P("vp"), P("dp", None, None)),
        check_vma=False,
    )
```

```python
import functools

import jax
import jax.numpy as jnp
from jax import lax
from jax.experimental import pallas as pl
from jax.experimental.pallas import tpu as pltpu
from jax.sharding import PartitionSpec as P

NUM_CLASSES = 21841
LN_EPS = 1e-5
F32 = jnp.float32
BF16 = jnp.bfloat16
MESH = pl.DeviceIdType.MESH


def pool_kernel(h_ref, gamma_ref, beta_ref, u_ref, stat_ref, acc_ref):
    tokens, rows, width = h_ref.shape
    lane = lax.broadcasted_iota(jnp.int32, (16, 128), 1)
    acc_ref[...] = jnp.zeros_like(acc_ref)
    stat_ref[...] = jnp.zeros_like(stat_ref)

    def group(i, carry):
        r0 = pl.multiple_of(i * 16, 16)
        here = pl.ds(r0, 16)
        for t in range(tokens):
            x = h_ref[t, here, :].astype(F32)
            m = x.sum(axis=-1, keepdims=True) * (1.0 / width)
            c = x - m
            r = lax.rsqrt((c * c).sum(axis=-1, keepdims=True) * (1.0 / width) + LN_EPS)
            acc_ref[here, :] += c * r
            stat_ref[here, :] = jnp.where(lane == t, m, jnp.where(lane == 64 + t, r, stat_ref[here, :]))
        return carry

    lax.fori_loop(0, rows // 16, group, 0)
    u = acc_ref[...] * (gamma_ref[...] * (1.0 / tokens)) + beta_ref[...]
    u_ref[...] = u.astype(BF16)


def pool_forward(ht, gamma, beta, rows=64):
    tokens, images, width = ht.shape
    rows = min(rows, images)
    return pl.pallas_call(
        pool_kernel,
        grid=(images // rows,),
        in_specs=[
            pl.BlockSpec((tokens, rows, width), lambda i: (0, i, 0)),
            pl.BlockSpec((1, width), lambda i: (0, 0)),
            pl.BlockSpec((1, width), lambda i: (0, 0)),
        ],
        out_specs=[
            pl.BlockSpec((rows, width), lambda i: (i, 0)),
            pl.BlockSpec((rows, 128), lambda i: (i, 0)),
        ],
        out_shape=[
            jax.ShapeDtypeStruct((images, width), BF16),
            jax.ShapeDtypeStruct((images, 128), F32),
        ],
        scratch_shapes=[pltpu.VMEM((rows, width), F32)],
        compiler_params=pltpu.CompilerParams(dimension_semantics=("arbitrary",)),
        cost_estimate=pl.CostEstimate(flops=8 * ht.size * 40, bytes_accessed=2 * ht.size, transcendentals=0),
        name="pool_forward",
    )(ht, gamma[None], beta[None])


def pool_backward_kernel(off_ref, h_ref, du_ref, stat_ref, gamma_ref, *rest):
    dh_ref, v_ref = rest[-2:]
    tokens, rows, width = h_ref.shape
    v = du_ref[...] * (gamma_ref[...] * (1.0 / tokens))
    v_ref[...] = v - v.sum(axis=-1, keepdims=True) * (1.0 / width)

    def group(i, carry):
        r0 = pl.multiple_of(i * 16, 16)
        here = pl.ds(r0, 16)
        for t in range(tokens):
            m = stat_ref[here, t : t + 1]
            r = stat_ref[here, 64 + t : 65 + t]
            xhat = (h_ref[t, here, :].astype(F32) - m) * r
            vc = v_ref[here, :]
            k = (vc * xhat).sum(axis=-1, keepdims=True) * (1.0 / width)
            dh_ref[t, here, :] = ((vc - xhat * k) * r).astype(BF16)
        return carry

    lax.fori_loop(0, rows // 16, group, 0)


def pool_backward(ht, du, stat, gamma, buf, block, rows=32):
    tokens, images, width = ht.shape
    count = du.shape[0]
    rows = min(rows, count)
    steps = count // rows
    in_specs = [
        pl.BlockSpec((tokens, rows, width), lambda i, o: (0, o[0] + i, 0)),
        pl.BlockSpec((rows, width), lambda i, o: (i, 0)),
        pl.BlockSpec((rows, 128), lambda i, o: (o[0] + i, 0)),
        pl.BlockSpec((1, width), lambda i, o: (0, 0)),
    ]
    args = [(block * steps).astype(jnp.int32)[None], ht, du, stat, gamma[None]]
    aliases = {}
    if buf is not None:
        in_specs.append(pl.BlockSpec(memory_space=pl.ANY))
        args.append(buf)
        aliases = {5: 0}
    return pl.pallas_call(
        pool_backward_kernel,
        grid_spec=pltpu.PrefetchScalarGridSpec(
            num_scalar_prefetch=1,
            grid=(steps,),
            in_specs=in_specs,
            out_specs=pl.BlockSpec((tokens, rows, width), lambda i, o: (0, o[0] + i, 0)),
            scratch_shapes=[pltpu.VMEM((rows, width), F32)],
        ),
        out_shape=jax.ShapeDtypeStruct((tokens, images, width), BF16),
        input_output_aliases=aliases,
        compiler_params=pltpu.CompilerParams(dimension_semantics=("arbitrary",)),
        cost_estimate=pl.CostEstimate(
            flops=40 * 12 * tokens * count * width, bytes_accessed=4 * tokens * count * width, transcendentals=0
        ),
        name="pool_backward",
    )(*args)


def place_kernel(off_ref, v_ref, o_ref):
    o_ref[...] = v_ref[...]


def place_first(v, block, total_rows, rows=32):
    count, n = v.shape
    steps = count // rows
    return pl.pallas_call(
        place_kernel,
        grid_spec=pltpu.PrefetchScalarGridSpec(
            num_scalar_prefetch=1,
            grid=(steps,),
            in_specs=[pl.BlockSpec((rows, n), lambda i, o: (i, 0))],
            out_specs=pl.BlockSpec((rows, n), lambda i, o: (o[0] + i, 0)),
        ),
        out_shape=jax.ShapeDtypeStruct((total_rows, n), v.dtype),
        cost_estimate=pl.CostEstimate(flops=10 * v.size, bytes_accessed=8 * v.size, transcendentals=0),
        name="place_first",
    )((block * steps).astype(jnp.int32)[None], v)


def head_kernel(
    n_glob, u_ref, b_ref, w_hbm, t_hbm,
    ra_hbm, pb_hbm, pc_hbm, pd_hbm, du_ref, db_ref,
    w_s, t_s, z_s, g_s, ut_s, m_s, s_s, ts_s, tz_s, stat_s, col_s, du_s, du_in,
    load_sem, stat_send, stat_recv, sib_send, sib_recv, far_sem, du_sem, out_sem, ready_sem,
):
    images, width = u_ref.shape
    classes = w_hbm.shape[1]
    padded = w_s.shape[1]
    chunk = 512
    n_chunks = padded // chunk
    tail = classes - (n_chunks - 1) * chunk
    part = width // 8
    half = images // 2

    vp = lax.axis_index("vp")
    dp = lax.axis_index("dp")
    core, x, y = lax.rem(dp, 2), lax.rem(dp // 2, 2), dp // 4
    p1 = jnp.where(core == 0, x, y)
    p2 = jnp.where(core == 0, y, x)
    sib = dp + 1 - 2 * core
    first = jnp.where(core == 0, dp + 2 - 4 * x, dp + 4 - 8 * y)
    z0 = lax.rem(vp, 2)
    near = vp + 1 - 2 * z0
    vp_size = stat_s.shape[0]
    others = [lax.rem(vp + k, vp_size) for k in range(1, vp_size)]

    barrier = pltpu.get_barrier_semaphore()
    for who in [(o, dp) for o in others] + [(vp, sib), (vp, first)]:
        pl.semaphore_signal(barrier, inc=1, device_id=who, device_id_type=MESH)

    def loads(i, n):
        cols = pl.ds(pl.multiple_of(i * chunk, chunk), n)
        return (
            pltpu.make_async_copy(w_hbm.at[:, cols], w_s.at[:, cols], load_sem.at[0, i]),
            pltpu.make_async_copy(t_hbm.at[:, cols], t_s.at[pl.ds(0, images), cols], load_sem.at[1, i]),
        )

    ahead = min(4, n_chunks - 1)
    for i in range(ahead):
        for c in loads(i, chunk):
            c.start()
    if padded > classes:
        w_s[:, classes:] = jnp.zeros((width, padded - classes), BF16)
        t_s[:, classes:] = jnp.zeros((t_s.shape[0], padded - classes), F32)
    m_s[...] = jnp.full_like(m_s, -jnp.inf)
    s_s[...] = jnp.zeros_like(s_s)
    ts_s[...] = jnp.zeros_like(ts_s)
    tz_s[...] = jnp.zeros_like(tz_s)
    limit = jnp.minimum(classes, NUM_CLASSES - vp * classes)

    def logits(i, carry):
        @pl.when(i + ahead < n_chunks - 1)
        def _():
            for c in loads(i + ahead, chunk):
                c.start()

        @pl.when(i + ahead == n_chunks - 1)
        def _():
            for c in loads(n_chunks - 1, tail):
                c.start()

        @pl.when(i < n_chunks - 1)
        def _():
            for c in loads(i, chunk):
                c.wait()

        @pl.when(i == n_chunks - 1)
        def _():
            for c in loads(n_chunks - 1, tail):
                c.wait()

        cols = pl.ds(pl.multiple_of(i * chunk, chunk), chunk)
        z = jnp.dot(u_ref[...], w_s[:, cols], preferred_element_type=F32) + b_ref[:, cols]
        valid = i * chunk + lax.broadcasted_iota(jnp.int32, (1, chunk), 1) < limit
        t = t_s[:images, cols]
        tz = t * jnp.where(valid, z, 0.0)
        z = jnp.where(valid, z, -jnp.inf)
        z_s[:images, cols] = z
        parts = [slice(k, k + 128) for k in range(0, chunk, 128)]
        m_old = m_s[...]
        m_new = m_old
        for p in parts:
            m_new = jnp.maximum(m_new, z[:, p])
        base = jnp.where(m_new == -jnp.inf, 0.0, m_new)
        s = s_s[...] * jnp.exp(m_old - base)
        ts = ts_s[...]
        tzs = tz_s[...]
        for p in parts:
            s += jnp.exp(z[:, p] - base)
            ts += t[:, p]
            tzs += tz[:, p]
        m_s[...] = m_new
        s_s[...] = s
        ts_s[...] = ts
        tz_s[...] = tzs
        return carry

    lax.fori_loop(0, n_chunks, logits, 0)

    m = m_s[...].max(axis=1, keepdims=True)
    s = (s_s[...] * jnp.exp(m_s[...] - m)).sum(axis=1, keepdims=True)
    ts = ts_s[...].sum(axis=1, keepdims=True)
    tz = tz_s[...].sum(axis=1, keepdims=True)
    lane = lax.broadcasted_iota(jnp.int32, m_s.shape, 1)
    packed = jnp.where(lane == 0, m, jnp.where(lane == 1, s, jnp.where(lane == 2, ts, tz)))
    stat_s[vp] = packed.T[:8]

    pl.semaphore_wait(barrier, vp_size + 1)
    copies = []
    for k, o in enumerate(others):
        c = pltpu.make_async_remote_copy(
            src_ref=stat_s.at[vp], dst_ref=stat_s.at[vp], send_sem=stat_send.at[k], recv_sem=stat_recv.at[k],
            device_id=(o, dp), device_id_type=MESH,
        )
        c.start()
        copies.append(c)
    ut_s[...] = u_ref[...].T
    for c in copies:
        c.wait()

    stat = [stat_s[k] for k in range(vp_size)]
    m = functools.reduce(jnp.maximum, [a[0:1] for a in stat])
    s = sum(a[1:2] * jnp.exp(a[0:1] - m) for a in stat)
    ts = sum(a[2:3] for a in stat)
    tz = sum(a[3:4] for a in stat)
    log_norm = m + jnp.log(s)
    loss = (log_norm * ts - tz).sum(axis=1, keepdims=True)
    row = lax.broadcasted_iota(jnp.int32, (128, m.shape[1]), 0)
    col_s[...] = jnp.where(row == 0, log_norm, ts).T

    def grads(i, carry):
        cols = pl.ds(pl.multiple_of(i * chunk, chunk), chunk)
        g = (jnp.exp(z_s[:images, cols] - col_s[:, 0:1]) * col_s[:, 1:2] - t_s[:images, cols]) * (1.0 / n_glob)
        g_s[:, cols] = g.astype(BF16)
        db_ref[:, cols] = g.sum(axis=0, keepdims=True)
        return carry

    lax.fori_loop(0, n_chunks, grads, 0)
    db_ref[:, classes:] = loss + jnp.zeros((1, padded - classes), F32)

    pl.semaphore_signal(ready_sem, inc=1, device_id=(vp, sib), device_id_type=MESH)

    def dots(src, n, dst, add):
        left = ut_s[pl.ds(pl.multiple_of(src * part, part), n), :]

        def body(i, carry):
            cols = pl.ds(pl.multiple_of(i * chunk, chunk), chunk)
            v = jnp.dot(left, g_s[:, cols], preferred_element_type=F32)
            at = pl.ds(dst, n)
            if add:
                t_s[at, cols] = t_s[at, cols] + v
            else:
                z_s[at, cols] = v
            return carry

        lax.fori_loop(0, n_chunks, body, 0)

    def to_sibling(k, at):
        rows = pl.ds(pl.multiple_of(at * part, part), part)
        return pltpu.make_async_remote_copy(
            src_ref=z_s.at[rows, pl.ds(0, classes)], dst_ref=t_s.at[pl.ds(k * part, part), pl.ds(0, classes)],
            send_sem=sib_send.at[k], recv_sem=sib_recv.at[k], device_id=(vp, sib), device_id_type=MESH,
        )

    sends = []
    for pair in range(2):
        dots(4 * (1 - core) + 2 * ((1 - p2) if pair == 0 else p2), 2 * part, pair * 2 * part, False)
        if pair == 0:
            pl.semaphore_wait(ready_sem, 1)
        for k in range(2):
            c = to_sibling(2 * pair + k, 2 * pair + ((1 - p1) if k == 0 else p1))
            c.start()
            sends.append(c)

    own = [4 * core + 2 * a + b for a, b in ((1 - p1, 1 - p2), (1 - p1, p2), (p1, 1 - p2), (p1, p2))]

    def piece(k):
        return t_s.at[pl.ds(k * part, part), pl.ds(0, classes)]

    sends[0].wait_recv()
    dots(own[0], part, 0, True)
    far = pltpu.make_async_remote_copy(
        src_ref=piece(0), dst_ref=ra_hbm, send_sem=far_sem.at[0], recv_sem=far_sem.at[1],
        device_id=(vp, first), device_id_type=MESH,
    )
    far.start()

    def du_dot(i, carry):
        cols = pl.ds(pl.multiple_of(i * chunk, chunk), chunk)
        v = lax.dot_general(g_s[:, cols], w_s[:, cols], (((1,), (1,)), ((), ())), preferred_element_type=F32)
        du_s[...] = du_s[...] + v
        return carry

    du_s[...] = jnp.zeros_like(du_s)
    lax.fori_loop(0, n_chunks, du_dot, 0)
    keep = pl.ds(pl.multiple_of(z0 * half, half), half)
    give = pl.ds(pl.multiple_of((1 - z0) * half, half), half)
    du_copy = pltpu.make_async_remote_copy(
        src_ref=du_s.at[give], dst_ref=du_in, send_sem=du_sem.at[0], recv_sem=du_sem.at[1],
        device_id=(near, dp), device_id_type=MESH,
    )
    du_copy.start()

    outs = []
    for k, out in ((1, pb_hbm), (2, pc_hbm), (3, pd_hbm)):
        sends[k].wait_recv()
        dots(own[k], part, k * part, True)
        c = pltpu.make_async_copy(piece(k), out, out_sem.at[k - 1])
        c.start()
        outs.append(c)
    for c in sends:
        c.wait_send()
    for c in outs:
        c.wait()
    du_copy.wait()
    du_ref[...] = du_s[keep, :] + du_in[...]
    far.wait()


def head(u, b, w, t, n_glob, vp_size):
    images, width = u.shape
    classes = w.shape[1]
    padded = (classes // 512 + 1) * 512
    part = width // 8
    rows = max(images, 4 * part)
    b = jnp.pad(b, (0, padded - classes))[None]
    any_spec = pl.BlockSpec(memory_space=pl.ANY)
    vmem = pl.BlockSpec(memory_space=pltpu.VMEM)
    dma = pltpu.SemaphoreType.DMA
    piece = jax.ShapeDtypeStruct((part, classes), F32)
    return pl.pallas_call(
        functools.partial(head_kernel, n_glob),
        in_specs=[vmem, vmem, any_spec, any_spec],
        out_specs=[any_spec] * 4 + [vmem] * 2,
        out_shape=[piece] * 4 + [
            jax.ShapeDtypeStruct((images // 2, width), F32),
            jax.ShapeDtypeStruct((1, padded), F32),
        ],
        scratch_shapes=[
            pltpu.VMEM((width, padded), BF16),
            pltpu.VMEM((rows, padded), F32),
            pltpu.VMEM((rows, padded), F32),
            pltpu.VMEM((images, padded), BF16),
            pltpu.VMEM((width, images), BF16),
        ] + [pltpu.VMEM((images, 128), F32)] * 4 + [
            pltpu.VMEM((vp_size, 8, images), F32),
            pltpu.VMEM((images, 128), F32),
            pltpu.VMEM((images, width), F32),
            pltpu.VMEM((images // 2, width), F32),
            dma((2, padded // 512)),
            dma((vp_size - 1,)),
            dma((vp_size - 1,)),
            dma((4,)),
            dma((4,)),
            dma((2,)),
            dma((2,)),
            dma((3,)),
            pltpu.SemaphoreType.REGULAR,
        ],
        compiler_params=pltpu.CompilerParams(
            collective_id=0, has_side_effects=True, vmem_limit_bytes=60 * 1024 * 1024
        ),
        cost_estimate=pl.CostEstimate(
            flops=6 * images * width * classes, bytes_accessed=20 * width * classes, transcendentals=0
        ),
        name="head",
    )(u, b, w, t)


def solution(mesh):
    dp_size = mesh.shape["dp"]
    vp_size = mesh.shape["vp"]
    sibling = [(i, i ^ 1) for i in range(8)]
    along_x = [(i, i ^ 2) for i in range(8)]
    along_y = [(i, i ^ 4) for i in range(8)]
    first = [(i, i ^ (4 if i & 1 else 2)) for i in range(8)]
    second = [(i, i ^ (2 if i & 1 else 4)) for i in range(8)]
    near = [(i, i ^ 1) for i in range(vp_size)]
    distant = [(i, i ^ 2) for i in range(vp_size)]

    def local_step(h_loc, gamma, beta, w_loc, b_loc, t_loc):
        images, _, width = h_loc.shape
        n_glob = images * dp_size
        classes = w_loc.shape[1]
        part = width // 8
        quarter = images // 4
        dp = lax.axis_index("dp")
        vp = lax.axis_index("vp")
        core, x, y = dp & 1, (dp >> 1) & 1, dp >> 2
        z0, z1 = vp & 1, vp >> 1
        p1 = jnp.where(core == 0, x, y)
        p2 = jnp.where(core == 0, y, x)
        own = [4 * core + 2 * a + b for a, b in ((1 - p1, 1 - p2), (1 - p1, p2), (p1, 1 - p2), (p1, p2))]
        sib = [4 * (1 - core) + 2 * a + b for a, b in ((1 - p2, 1 - p1), (1 - p2, p1), (p2, 1 - p1), (p2, p1))]

        ht = h_loc.transpose(1, 0, 2)
        u, stat = pool_forward(ht, gamma, beta)
        r_c, b, c, d, du_half, db = head(u, b_loc, w_loc, t_loc, n_glob, vp_size)

        def send(v, pairs):
            return lax.ppermute(v, "dp", pairs)

        r_d = send(b, first)
        c = c + r_c
        r_d2 = send(c, second)

        got = lax.ppermute(lax.dynamic_slice(du_half, ((1 - z1) * quarter, 0), (quarter, width)), "vp", distant)
        du_own = lax.dynamic_slice(du_half, (z1 * quarter, 0), (quarter, width)) + got
        du_far = lax.ppermute(du_own, "vp", distant)
        du_near = lax.ppermute(du_own, "vp", near)
        du_last = lax.ppermute(du_far, "vp", near)

        for pairs in (sibling, along_x, along_y):
            db = db + send(db, pairs)

        d = (d + r_d) + r_d2
        c_fin = send(d, second)
        b_fin = send(d, first)
        a_fin = send(c_fin, first)
        mine = [a_fin, b_fin, c_fin, d]
        theirs = [send(v, sibling) for v in mine]

        dh = None
        for v, k in (
            (du_own, 2 * z0 + z1),
            (du_far, 2 * z0 + 1 - z1),
            (du_near, 2 * (1 - z0) + z1),
            (du_last, 2 * (1 - z0) + 1 - z1),
        ):
            dh = pool_backward(ht, v, stat, gamma, dh, k)

        out = place_first(d, own[3], width)
        for v, k in ((theirs[3], sib[3]), (mine[2], own[2]), (theirs[2], sib[2]),
                     (mine[1], own[1]), (theirs[1], sib[1]), (mine[0], own[0]), (theirs[0], sib[0])):
            out = lax.dynamic_update_slice(out, v, (k * part, 0))
        return db[0, classes] / n_glob, out, db[0, :classes], dh.transpose(1, 0, 2)

    return jax.shard_map(
        local_step,
        mesh=mesh,
        in_specs=(P("dp", None, None), P(), P(), P(None, "vp"), P("vp"), P("dp", "vp")),
        out_specs=(P(), P(None, "vp"), P("vp"), P("dp", None, None)),
        check_vma=False,
    )
```

```python
import functools

import jax
import jax.numpy as jnp
from jax import lax
from jax.experimental import pallas as pl
from jax.experimental.pallas import tpu as pltpu
from jax.sharding import PartitionSpec as P


NUM_CLASSES = 21841
LN_EPS = 1e-5
F32 = jnp.float32
BF16 = jnp.bfloat16
MESH = pl.DeviceIdType.MESH


def norm_rows(x):
    width = x.shape[-1]
    c = x - x.sum(axis=-1, keepdims=True) * (1.0 / width)
    var = (c * c).sum(axis=-1, keepdims=True) * (1.0 / width)
    return c, lax.rsqrt(var + LN_EPS)


def pool_kernel(h_ref, gamma_ref, beta_ref, u_ref, acc_ref):
    tokens, rows, _ = h_ref.shape
    acc_ref[...] = jnp.zeros_like(acc_ref)

    def group(i, carry):
        here = pl.ds(pl.multiple_of(i * 16, 16), 16)
        for t in range(tokens):
            c, r = norm_rows(h_ref[t, here, :].astype(F32))
            acc_ref[here, :] += c * r
        return carry

    lax.fori_loop(0, rows // 16, group, 0)
    u = acc_ref[...] * (gamma_ref[...] * (1.0 / tokens)) + beta_ref[...]
    u_ref[...] = u.astype(BF16)


def pool_forward(ht, gamma, beta, rows=32):
    tokens, images, width = ht.shape
    rows = min(rows, images)
    return pl.pallas_call(
        pool_kernel,
        grid=(images // rows,),
        in_specs=[
            pl.BlockSpec((tokens, rows, width), lambda i: (0, i, 0)),
            pl.BlockSpec((1, width), lambda i: (0, 0)),
            pl.BlockSpec((1, width), lambda i: (0, 0)),
        ],
        out_specs=pl.BlockSpec((rows, width), lambda i: (i, 0)),
        out_shape=jax.ShapeDtypeStruct((images, width), BF16),
        scratch_shapes=[pltpu.VMEM((rows, width), F32)],
        compiler_params=pltpu.CompilerParams(dimension_semantics=("arbitrary",)),
        cost_estimate=pl.CostEstimate(flops=8 * ht.size * 40, bytes_accessed=2 * ht.size, transcendentals=0),
        name="pool_forward",
    )(ht, gamma[None], beta[None])


def pool_backward_kernel(off_ref, h_ref, du_ref, gamma_ref, *rest):
    dh_ref, token_ref, v_ref = rest[-3:]
    tokens, rows, width = h_ref.shape
    v = du_ref[...] * (gamma_ref[...] * (1.0 / tokens))
    v_ref[...] = v - v.sum(axis=-1, keepdims=True) * (1.0 / width)
    token_ref[...] = jnp.zeros_like(token_ref)

    def group(i, carry):
        here = pl.ds(pl.multiple_of(i * 16, 16), 16)
        for t in range(tokens):
            c, r = norm_rows(h_ref[t, here, :].astype(F32))
            vc = v_ref[here, :]
            xhat = c * r
            k = (vc * xhat).sum(axis=-1, keepdims=True) * (1.0 / width)
            dh_ref[t, here, :] = ((vc - xhat * k) * r).astype(BF16)
        return carry

    lax.fori_loop(0, rows // 16, group, 0)


def pool_backward(ht, du, gamma, buf, block, after, rows=32):
    tokens, images, width = ht.shape
    count = du.shape[0]
    rows = min(rows, count)
    steps = count // rows
    any_spec = pl.BlockSpec(memory_space=pl.ANY)
    in_specs = [
        pl.BlockSpec((tokens, rows, width), lambda i, o: (0, o[0] + i, 0)),
        pl.BlockSpec((rows, width), lambda i, o: (i, 0)),
        pl.BlockSpec((1, width), lambda i, o: (0, 0)),
        any_spec,
    ]
    args = [(block * steps).astype(jnp.int32)[None], ht, du, gamma[None], after]
    aliases = {}
    if buf is not None:
        in_specs.append(any_spec)
        args.append(buf)
        aliases = {5: 0}
    return pl.pallas_call(
        pool_backward_kernel,
        grid_spec=pltpu.PrefetchScalarGridSpec(
            num_scalar_prefetch=1,
            grid=(steps,),
            in_specs=in_specs,
            out_specs=[
                pl.BlockSpec((tokens, rows, width), lambda i, o: (0, o[0] + i, 0)),
                pl.BlockSpec((8, 128), lambda i, o: (0, 0)),
            ],
            scratch_shapes=[pltpu.VMEM((rows, width), F32)],
        ),
        out_shape=[
            jax.ShapeDtypeStruct((tokens, images, width), BF16),
            jax.ShapeDtypeStruct((8, 128), F32),
        ],
        input_output_aliases=aliases,
        compiler_params=pltpu.CompilerParams(dimension_semantics=("arbitrary",)),
        cost_estimate=pl.CostEstimate(
            flops=40 * 12 * tokens * count * width, bytes_accessed=4 * tokens * count * width, transcendentals=0
        ),
        name="pool_backward",
    )(*args)


def add_kernel(a_ref, b_ref, c_ref, *rest):
    rest[-1][...] = (a_ref[...] + b_ref[...]) + c_ref[...]


def add_after(a, b, c, *after, rows=32):
    n = a.shape[1]
    spec = pl.BlockSpec((rows, n), lambda i: (i, 0))
    return pl.pallas_call(
        add_kernel,
        grid=(a.shape[0] // rows,),
        in_specs=[spec] * 3 + [pl.BlockSpec(memory_space=pl.ANY)] * len(after),
        out_specs=spec,
        out_shape=jax.ShapeDtypeStruct(a.shape, a.dtype),
        cost_estimate=pl.CostEstimate(flops=10 * a.size, bytes_accessed=16 * a.size, transcendentals=0),
        name="add_after",
    )(a, b, c, *after)


def place_kernel(off_ref, v_ref, o_ref):
    o_ref[...] = v_ref[...]


def place_first(v, block, total_rows, rows=32):
    count, n = v.shape
    steps = count // rows
    return pl.pallas_call(
        place_kernel,
        grid_spec=pltpu.PrefetchScalarGridSpec(
            num_scalar_prefetch=1,
            grid=(steps,),
            in_specs=[pl.BlockSpec((rows, n), lambda i, o: (i, 0))],
            out_specs=pl.BlockSpec((rows, n), lambda i, o: (o[0] + i, 0)),
        ),
        out_shape=jax.ShapeDtypeStruct((total_rows, n), v.dtype),
        cost_estimate=pl.CostEstimate(flops=10 * v.size, bytes_accessed=8 * v.size, transcendentals=0),
        name="place_first",
    )((block * steps).astype(jnp.int32)[None], v)


def head_kernel(
    n_glob, u_ref, b_ref, w_hbm, t_hbm,
    pb_hbm, pc_hbm, pd_hbm, du_ref, db_ref,
    w_s, t_s, z_s, ra_s, b_s, g_s, ut_s, m_s, s_s, ts_s, tz_s, stat_s, col_s, du_s, du_in,
    load_sem, stat_send, stat_recv, sib_send, sib_recv, far_sem, du_sem, out_sem, ready_sem,
):
    images, width = u_ref.shape
    classes = w_hbm.shape[1]
    padded = w_s.shape[1]
    chunk = 512
    n_chunks = padded // chunk
    tail = classes - (n_chunks - 1) * chunk
    part = width // 8
    half = images // 2

    vp = lax.axis_index("vp")
    dp = lax.axis_index("dp")
    core, x, y = lax.rem(dp, 2), lax.rem(dp // 2, 2), dp // 4
    p1 = jnp.where(core == 0, x, y)
    p2 = jnp.where(core == 0, y, x)
    sib = dp + 1 - 2 * core
    first = jnp.where(core == 0, dp + 2 - 4 * x, dp + 4 - 8 * y)
    z0 = lax.rem(vp, 2)
    near = vp + 1 - 2 * z0
    vp_size = stat_s.shape[0]
    others = [lax.rem(vp + k, vp_size) for k in range(1, vp_size)]

    barrier = pltpu.get_barrier_semaphore()
    for who in [(o, dp) for o in others] + [(vp, sib), (vp, first)]:
        pl.semaphore_signal(barrier, inc=1, device_id=who, device_id_type=MESH)

    def loads(i, n):
        cols = pl.ds(pl.multiple_of(i * chunk, chunk), n)
        return (
            pltpu.make_async_copy(w_hbm.at[:, cols], w_s.at[:, cols], load_sem.at[0, i]),
            pltpu.make_async_copy(t_hbm.at[:, cols], t_s.at[pl.ds(0, images), cols], load_sem.at[1, i]),
        )

    ahead = min(4, n_chunks - 1)
    for i in range(ahead):
        for c in loads(i, chunk):
            c.start()
    if padded > classes:
        b_s[:, classes:] = jnp.zeros((1, padded - classes), F32)
        w_s[:, classes:] = jnp.zeros((width, padded - classes), BF16)
        t_s[:, classes:] = jnp.zeros((t_s.shape[0], padded - classes), F32)
    b_s[:, :classes] = b_ref[...]
    m_s[...] = jnp.full_like(m_s, -jnp.inf)
    s_s[...] = jnp.zeros_like(s_s)
    ts_s[...] = jnp.zeros_like(ts_s)
    tz_s[...] = jnp.zeros_like(tz_s)
    limit = jnp.minimum(classes, NUM_CLASSES - vp * classes)

    def logits(i, carry):
        @pl.when(i + ahead < n_chunks - 1)
        def _():
            for c in loads(i + ahead, chunk):
                c.start()

        @pl.when(i + ahead == n_chunks - 1)
        def _():
            for c in loads(n_chunks - 1, tail):
                c.start()

        @pl.when(i < n_chunks - 1)
        def _():
            for c in loads(i, chunk):
                c.wait()

        @pl.when(i == n_chunks - 1)
        def _():
            for c in loads(n_chunks - 1, tail):
                c.wait()

        cols = pl.ds(pl.multiple_of(i * chunk, chunk), chunk)
        z = jnp.dot(u_ref[...], w_s[:, cols], preferred_element_type=F32) + b_s[:, cols]
        valid = i * chunk + lax.broadcasted_iota(jnp.int32, (1, chunk), 1) < limit
        t = t_s[:images, cols]
        tz = t * jnp.where(valid, z, 0.0)
        z = jnp.where(valid, z, -jnp.inf)
        z_s[:images, cols] = z
        parts = [slice(k, k + 128) for k in range(0, chunk, 128)]
        m_old = m_s[...]
        m_new = m_old
        for p in parts:
            m_new = jnp.maximum(m_new, z[:, p])
        base = jnp.where(m_new == -jnp.inf, 0.0, m_new)
        s = s_s[...] * jnp.exp(m_old - base)
        ts = ts_s[...]
        tzs = tz_s[...]
        for p in parts:
            s += jnp.exp(z[:, p] - base)
            ts += t[:, p]
            tzs += tz[:, p]
        m_s[...] = m_new
        s_s[...] = s
        ts_s[...] = ts
        tz_s[...] = tzs
        return carry

    lax.fori_loop(0, n_chunks, logits, 0)

    m = m_s[...].max(axis=1, keepdims=True)
    s = (s_s[...] * jnp.exp(m_s[...] - m)).sum(axis=1, keepdims=True)
    ts = ts_s[...].sum(axis=1, keepdims=True)
    tz = tz_s[...].sum(axis=1, keepdims=True)
    lane = lax.broadcasted_iota(jnp.int32, m_s.shape, 1)
    packed = jnp.where(lane == 0, m, jnp.where(lane == 1, s, jnp.where(lane == 2, ts, tz)))
    stat_s[vp] = packed.T[:8]

    pl.semaphore_wait(barrier, vp_size + 1)
    copies = []
    for k, o in enumerate(others):
        c = pltpu.make_async_remote_copy(
            src_ref=stat_s.at[vp], dst_ref=stat_s.at[vp], send_sem=stat_send.at[k], recv_sem=stat_recv.at[k],
            device_id=(o, dp), device_id_type=MESH,
        )
        c.start()
        copies.append(c)
    ut_s[...] = u_ref[...].T
    for c in copies:
        c.wait()

    stat = [stat_s[k] for k in range(vp_size)]
    m = functools.reduce(jnp.maximum, [a[0:1] for a in stat])
    s = sum(a[1:2] * jnp.exp(a[0:1] - m) for a in stat)
    ts = sum(a[2:3] for a in stat)
    tz = sum(a[3:4] for a in stat)
    log_norm = m + jnp.log(s)
    loss = (log_norm * ts - tz).sum(axis=1, keepdims=True)
    row = lax.broadcasted_iota(jnp.int32, (128, m.shape[1]), 0)
    col_s[...] = jnp.where(row == 0, log_norm, ts).T

    def grads(i, carry):
        cols = pl.ds(pl.multiple_of(i * chunk, chunk), chunk)
        g = (jnp.exp(z_s[:images, cols] - col_s[:, 0:1]) * col_s[:, 1:2] - t_s[:images, cols]) * (1.0 / n_glob)
        g_s[:, cols] = g.astype(BF16)
        db_ref[:, cols] = g.sum(axis=0, keepdims=True)
        return carry

    lax.fori_loop(0, n_chunks, grads, 0)
    db_ref[:, classes:] = loss + jnp.zeros((1, padded - classes), F32)

    pl.semaphore_signal(ready_sem, inc=1, device_id=(vp, sib), device_id_type=MESH)

    def dots(src, n, dst, add):
        left = ut_s[pl.ds(pl.multiple_of(src * part, part), n), :]

        def body(i, carry):
            cols = pl.ds(pl.multiple_of(i * chunk, chunk), chunk)
            v = jnp.dot(left, g_s[:, cols], preferred_element_type=F32)
            at = pl.ds(dst, n)
            if add:
                t_s[at, cols] = t_s[at, cols] + v
            else:
                z_s[at, cols] = v
            return carry

        lax.fori_loop(0, n_chunks, body, 0)

    def to_sibling(k, at):
        rows = pl.ds(pl.multiple_of(at * part, part), part)
        return pltpu.make_async_remote_copy(
            src_ref=z_s.at[rows, pl.ds(0, classes)], dst_ref=t_s.at[pl.ds(k * part, part), pl.ds(0, classes)],
            send_sem=sib_send.at[k], recv_sem=sib_recv.at[k], device_id=(vp, sib), device_id_type=MESH,
        )

    dots(4 * (1 - core) + 2 * (1 - p2), 2 * part, 0, False)
    sends = [to_sibling(0, 1 - p1), to_sibling(1, p1), to_sibling(2, 3 - p1), to_sibling(3, 2 + p1)]
    pl.semaphore_wait(ready_sem, 1)
    sends[0].start()
    dots(4 * (1 - core) + 2 * p2, 2 * part, 2 * part, False)
    sends[1].start()

    own = [4 * core + 2 * a + b for a, b in ((1 - p1, 1 - p2), (1 - p1, p2), (p1, 1 - p2), (p1, p2))]

    def piece(k):
        return t_s.at[pl.ds(k * part, part), pl.ds(0, classes)]

    sends[0].wait_recv()
    sends[2].start()
    sends[3].start()
    dots(own[0], part, 0, True)
    far = pltpu.make_async_remote_copy(
        src_ref=piece(0), dst_ref=ra_s, send_sem=far_sem.at[0], recv_sem=far_sem.at[1],
        device_id=(vp, first), device_id_type=MESH,
    )
    far.start()

    def du_dot(i, carry):
        cols = pl.ds(pl.multiple_of(i * chunk, chunk), chunk)
        v = lax.dot_general(g_s[:, cols], w_s[:, cols], (((1,), (1,)), ((), ())), preferred_element_type=F32)
        du_s[...] = du_s[...] + v
        return carry

    du_s[...] = jnp.zeros_like(du_s)
    lax.fori_loop(0, n_chunks, du_dot, 0)
    keep = pl.ds(pl.multiple_of(z0 * half, half), half)
    give = pl.ds(pl.multiple_of((1 - z0) * half, half), half)
    du_copy = pltpu.make_async_remote_copy(
        src_ref=du_s.at[give], dst_ref=du_in, send_sem=du_sem.at[0], recv_sem=du_sem.at[1],
        device_id=(near, dp), device_id_type=MESH,
    )
    du_copy.start()

    outs = []
    for k, out in ((1, pb_hbm), (2, pc_hbm), (3, pd_hbm)):
        sends[k].wait_recv()
        dots(own[k], part, k * part, True)
        c = pltpu.make_async_copy(piece(k), out, out_sem.at[k - 1])
        if k != 2:
            c.start()
        outs.append(c)
    for c in sends:
        c.wait_send()
    du_copy.wait()
    du_ref[...] = du_s[keep, :] + du_in[...]
    far.wait()

    def add_far(i, carry):
        cols = pl.ds(pl.multiple_of(i * 128, 128), 128)
        at = pl.ds(2 * part, part)
        t_s[at, cols] = t_s[at, cols] + ra_s[:, cols]
        return carry

    lax.fori_loop(0, classes // 128, add_far, 0)
    outs[1].start()
    for c in outs:
        c.wait()


def head(u, b, w, t, n_glob, vp_size):
    images, width = u.shape
    classes = w.shape[1]
    padded = (classes // 512 + 1) * 512
    part = width // 8
    rows = max(images, 4 * part)
    any_spec = pl.BlockSpec(memory_space=pl.ANY)
    vmem = pl.BlockSpec(memory_space=pltpu.VMEM)
    dma = pltpu.SemaphoreType.DMA
    piece = jax.ShapeDtypeStruct((part, classes), F32)
    return pl.pallas_call(
        functools.partial(head_kernel, n_glob),
        in_specs=[vmem, vmem, any_spec, any_spec],
        out_specs=[any_spec] * 3 + [vmem] * 2,
        out_shape=[piece] * 3 + [
            jax.ShapeDtypeStruct((images // 2, width), F32),
            jax.ShapeDtypeStruct((1, padded), F32),
        ],
        scratch_shapes=[
            pltpu.VMEM((width, padded), BF16),
            pltpu.VMEM((rows, padded), F32),
            pltpu.VMEM((rows, padded), F32),
            pltpu.VMEM((part, classes), F32),
            pltpu.VMEM((1, padded), F32),
            pltpu.VMEM((images, padded), BF16),
            pltpu.VMEM((width, images), BF16),
        ] + [pltpu.VMEM((images, 128), F32)] * 4 + [
            pltpu.VMEM((vp_size, 8, images), F32),
            pltpu.VMEM((images, 128), F32),
            pltpu.VMEM((images, width), F32),
            pltpu.VMEM((images // 2, width), F32),
            dma((2, padded // 512)),
            dma((vp_size - 1,)),
            dma((vp_size - 1,)),
            dma((4,)),
            dma((4,)),
            dma((2,)),
            dma((2,)),
            dma((3,)),
            pltpu.SemaphoreType.REGULAR,
        ],
        compiler_params=pltpu.CompilerParams(
            collective_id=0, has_side_effects=True, vmem_limit_bytes=60 * 1024 * 1024
        ),
        cost_estimate=pl.CostEstimate(
            flops=6 * images * width * classes, bytes_accessed=20 * width * classes, transcendentals=0
        ),
        name="head",
    )(u, b[None], w, t)


def solution(mesh):
    dp_size = mesh.shape["dp"]
    vp_size = mesh.shape["vp"]
    sibling = [(i, i ^ 1) for i in range(8)]
    along_x = [(i, i ^ 2) for i in range(8)]
    along_y = [(i, i ^ 4) for i in range(8)]
    first = [(i, i ^ (4 if i & 1 else 2)) for i in range(8)]
    second = [(i, i ^ (2 if i & 1 else 4)) for i in range(8)]
    near = [(i, i ^ 1) for i in range(vp_size)]
    distant = [(i, i ^ 2) for i in range(vp_size)]

    def local_step(h_loc, gamma, beta, w_loc, b_loc, t_loc):
        images, _, width = h_loc.shape
        n_glob = images * dp_size
        classes = w_loc.shape[1]
        part = width // 8
        quarter = images // 4
        dp = lax.axis_index("dp")
        vp = lax.axis_index("vp")
        core, x, y = dp & 1, (dp >> 1) & 1, dp >> 2
        z0, z1 = vp & 1, vp >> 1
        p1 = jnp.where(core == 0, x, y)
        p2 = jnp.where(core == 0, y, x)
        own = [4 * core + 2 * a + b for a, b in ((1 - p1, 1 - p2), (1 - p1, p2), (p1, 1 - p2), (p1, p2))]
        sib = [4 * (1 - core) + 2 * a + b for a, b in ((1 - p2, 1 - p1), (1 - p2, p1), (p2, 1 - p1), (p2, p1))]

        ht = h_loc.transpose(1, 0, 2)
        u = pool_forward(ht, gamma, beta)
        b, c, d, du_half, db = head(u, b_loc, w_loc, t_loc, n_glob, vp_size)

        def send(v, pairs):
            return lax.ppermute(v, "dp", pairs)

        r_d = send(b, first)
        r_d2 = send(c, second)

        got = lax.ppermute(lax.dynamic_slice(du_half, ((1 - z1) * quarter, 0), (quarter, width)), "vp", distant)
        du_own = lax.dynamic_slice(du_half, (z1 * quarter, 0), (quarter, width)) + got
        du_far = lax.ppermute(du_own, "vp", distant)
        du_near = lax.ppermute(du_own, "vp", near)
        du_last = lax.ppermute(du_far, "vp", near)

        for pairs in (sibling, along_x, along_y):
            db = db + send(db, pairs)

        dh, token = pool_backward(ht, du_own, gamma, None, 2 * z0 + z1, db)
        dh, token = pool_backward(ht, du_far, gamma, dh, 2 * z0 + 1 - z1, token)
        d = add_after(d, r_d, r_d2, token, du_near)
        c_fin = send(d, second)
        b_fin = send(d, first)
        dh, token = pool_backward(ht, du_near, gamma, dh, 2 * (1 - z0) + z1, d)
        dh, token = pool_backward(ht, du_last, gamma, dh, 2 * (1 - z0) + 1 - z1, token)
        a_fin = send(c_fin, first)
        mine = [a_fin, b_fin, c_fin, d]
        theirs = [send(v, sibling) for v in mine]

        out = place_first(d, own[3], width)
        for v, k in ((theirs[3], sib[3]), (mine[2], own[2]), (theirs[2], sib[2]),
                     (mine[1], own[1]), (theirs[1], sib[1]), (mine[0], own[0]), (theirs[0], sib[0])):
            out = lax.dynamic_update_slice(out, v, (k * part, 0))
        return db[0, classes] / n_glob, out, db[0, :classes], dh.transpose(1, 0, 2)

    return jax.shard_map(
        local_step,
        mesh=mesh,
        in_specs=(P("dp", None, None), P(), P(), P(None, "vp"), P("vp"), P("dp", "vp")),
        out_specs=(P(), P(None, "vp"), P("vp"), P("dp", None, None)),
        check_vma=False,
    )
```

```python
import functools

import jax
import jax.numpy as jnp
from jax import lax
from jax.experimental import pallas as pl
from jax.experimental.pallas import tpu as pltpu
from jax.sharding import PartitionSpec as P


NUM_CLASSES = 21841
LN_EPS = 1e-5
F32 = jnp.float32
BF16 = jnp.bfloat16
MESH = pl.DeviceIdType.MESH


def norm_rows(x):
    width = x.shape[-1]
    c = x - x.sum(axis=-1, keepdims=True) * (1.0 / width)
    var = (c * c).sum(axis=-1, keepdims=True) * (1.0 / width)
    return c, lax.rsqrt(var + LN_EPS)


def pool_kernel(h_ref, gamma_ref, beta_ref, u_ref, acc_ref):
    tokens, rows, _ = h_ref.shape
    acc_ref[...] = jnp.zeros_like(acc_ref)

    def group(i, carry):
        here = pl.ds(pl.multiple_of(i * 16, 16), 16)
        for t in range(tokens):
            c, r = norm_rows(h_ref[t, here, :].astype(F32))
            acc_ref[here, :] += c * r
        return carry

    lax.fori_loop(0, rows // 16, group, 0)
    u = acc_ref[...] * (gamma_ref[...] * (1.0 / tokens)) + beta_ref[...]
    u_ref[...] = u.astype(BF16)


def pool_forward(ht, gamma, beta, rows=32):
    tokens, images, width = ht.shape
    rows = min(rows, images)
    return pl.pallas_call(
        pool_kernel,
        grid=(images // rows,),
        in_specs=[
            pl.BlockSpec((tokens, rows, width), lambda i: (0, i, 0)),
            pl.BlockSpec((1, width), lambda i: (0, 0)),
            pl.BlockSpec((1, width), lambda i: (0, 0)),
        ],
        out_specs=pl.BlockSpec((rows, width), lambda i: (i, 0)),
        out_shape=jax.ShapeDtypeStruct((images, width), BF16),
        scratch_shapes=[pltpu.VMEM((rows, width), F32)],
        compiler_params=pltpu.CompilerParams(dimension_semantics=("arbitrary",)),
        cost_estimate=pl.CostEstimate(flops=8 * ht.size * 40, bytes_accessed=2 * ht.size, transcendentals=0),
        name="pool_forward",
    )(ht, gamma[None], beta[None])


def pool_backward_kernel(off_ref, h_ref, du_ref, gamma_ref, *rest):
    dh_ref, token_ref, v_ref = rest[-3:]
    tokens, rows, width = h_ref.shape
    v = du_ref[...] * (gamma_ref[...] * (1.0 / tokens))
    v_ref[...] = v - v.sum(axis=-1, keepdims=True) * (1.0 / width)
    token_ref[...] = jnp.zeros_like(token_ref)

    def group(i, carry):
        here = pl.ds(pl.multiple_of(i * 16, 16), 16)
        for t in range(tokens):
            c, r = norm_rows(h_ref[t, here, :].astype(F32))
            vc = v_ref[here, :]
            xhat = c * r
            k = (vc * xhat).sum(axis=-1, keepdims=True) * (1.0 / width)
            dh_ref[t, here, :] = ((vc - xhat * k) * r).astype(BF16)
        return carry

    lax.fori_loop(0, rows // 16, group, 0)


def pool_backward(ht, du, gamma, buf, block, after, rows=32):
    tokens, images, width = ht.shape
    count = du.shape[0]
    rows = min(rows, count)
    steps = count // rows
    any_spec = pl.BlockSpec(memory_space=pl.ANY)
    in_specs = [
        pl.BlockSpec((tokens, rows, width), lambda i, o: (0, o[0] + i, 0)),
        pl.BlockSpec((rows, width), lambda i, o: (i, 0)),
        pl.BlockSpec((1, width), lambda i, o: (0, 0)),
        any_spec,
    ]
    args = [(block * steps).astype(jnp.int32)[None], ht, du, gamma[None], after]
    aliases = {}
    if buf is not None:
        in_specs.append(any_spec)
        args.append(buf)
        aliases = {5: 0}
    return pl.pallas_call(
        pool_backward_kernel,
        grid_spec=pltpu.PrefetchScalarGridSpec(
            num_scalar_prefetch=1,
            grid=(steps,),
            in_specs=in_specs,
            out_specs=[
                pl.BlockSpec((tokens, rows, width), lambda i, o: (0, o[0] + i, 0)),
                pl.BlockSpec((8, 128), lambda i, o: (0, 0)),
            ],
            scratch_shapes=[pltpu.VMEM((rows, width), F32)],
        ),
        out_shape=[
            jax.ShapeDtypeStruct((tokens, images, width), BF16),
            jax.ShapeDtypeStruct((8, 128), F32),
        ],
        input_output_aliases=aliases,
        compiler_params=pltpu.CompilerParams(dimension_semantics=("arbitrary",)),
        cost_estimate=pl.CostEstimate(
            flops=40 * 12 * tokens * count * width, bytes_accessed=4 * tokens * count * width, transcendentals=0
        ),
        name="pool_backward",
    )(*args)


def place_kernel(off_ref, v_ref, o_ref):
    o_ref[...] = v_ref[...]


def place_first(v, block, total_rows, rows=32):
    count, n = v.shape
    steps = count // rows
    return pl.pallas_call(
        place_kernel,
        grid_spec=pltpu.PrefetchScalarGridSpec(
            num_scalar_prefetch=1,
            grid=(steps,),
            in_specs=[pl.BlockSpec((rows, n), lambda i, o: (i, 0))],
            out_specs=pl.BlockSpec((rows, n), lambda i, o: (o[0] + i, 0)),
        ),
        out_shape=jax.ShapeDtypeStruct((total_rows, n), v.dtype),
        cost_estimate=pl.CostEstimate(flops=10 * v.size, bytes_accessed=8 * v.size, transcendentals=0),
        name="place_first",
    )((block * steps).astype(jnp.int32)[None], v)


def head_kernel(
    n_glob, u_ref, b_ref, w_hbm, t_hbm,
    pb_hbm, pc_hbm, pd_hbm, du_ref, db_ref,
    w_s, t_s, z_s, ra_s, b_s, db_s, g_s, ut_s, m_s, s_s, ts_s, tz_s, stat_s, col_s, du_s, du_in,
    load_sem, stat_send, stat_recv, sib_send, sib_recv, far_sem, du_sem, db_send, db_recv, out_sem, ready_sem,
):
    images, width = u_ref.shape
    classes = w_hbm.shape[1]
    padded = w_s.shape[1]
    chunk = 512
    n_chunks = padded // chunk
    tail = classes - (n_chunks - 1) * chunk
    part = width // 8
    half = images // 2

    vp = lax.axis_index("vp")
    dp = lax.axis_index("dp")
    core, x, y = lax.rem(dp, 2), lax.rem(dp // 2, 2), dp // 4
    p1 = jnp.where(core == 0, x, y)
    p2 = jnp.where(core == 0, y, x)
    sib = dp + 1 - 2 * core
    along_x, along_y = dp + 2 - 4 * x, dp + 4 - 8 * y
    first = jnp.where(core == 0, along_x, along_y)
    z0 = lax.rem(vp, 2)
    near = vp + 1 - 2 * z0
    vp_size = stat_s.shape[0]
    others = [lax.rem(vp + k, vp_size) for k in range(1, vp_size)]

    barrier = pltpu.get_barrier_semaphore()
    for who in [(o, dp) for o in others] + [(vp, sib), (vp, along_x), (vp, along_y)]:
        pl.semaphore_signal(barrier, inc=1, device_id=who, device_id_type=MESH)

    def loads(i, n):
        cols = pl.ds(pl.multiple_of(i * chunk, chunk), n)
        return (
            pltpu.make_async_copy(w_hbm.at[:, cols], w_s.at[:, cols], load_sem.at[0, i]),
            pltpu.make_async_copy(t_hbm.at[:, cols], t_s.at[pl.ds(0, images), cols], load_sem.at[1, i]),
        )

    ahead = min(4, n_chunks - 1)
    for i in range(ahead):
        for c in loads(i, chunk):
            c.start()
    if padded > classes:
        b_s[:, classes:] = jnp.zeros((1, padded - classes), F32)
        w_s[:, classes:] = jnp.zeros((width, padded - classes), BF16)
        t_s[:, classes:] = jnp.zeros((t_s.shape[0], padded - classes), F32)
    b_s[:, :classes] = b_ref[...]
    m_s[...] = jnp.full_like(m_s, -jnp.inf)
    s_s[...] = jnp.zeros_like(s_s)
    ts_s[...] = jnp.zeros_like(ts_s)
    tz_s[...] = jnp.zeros_like(tz_s)
    limit = jnp.minimum(classes, NUM_CLASSES - vp * classes)

    def logits(i, carry):
        @pl.when(i + ahead < n_chunks - 1)
        def _():
            for c in loads(i + ahead, chunk):
                c.start()

        @pl.when(i + ahead == n_chunks - 1)
        def _():
            for c in loads(n_chunks - 1, tail):
                c.start()

        @pl.when(i < n_chunks - 1)
        def _():
            for c in loads(i, chunk):
                c.wait()

        @pl.when(i == n_chunks - 1)
        def _():
            for c in loads(n_chunks - 1, tail):
                c.wait()

        cols = pl.ds(pl.multiple_of(i * chunk, chunk), chunk)
        z = jnp.dot(u_ref[...], w_s[:, cols], preferred_element_type=F32) + b_s[:, cols]
        valid = i * chunk + lax.broadcasted_iota(jnp.int32, (1, chunk), 1) < limit
        t = t_s[:images, cols]
        tz = t * jnp.where(valid, z, 0.0)
        z = jnp.where(valid, z, -jnp.inf)
        z_s[:images, cols] = z
        parts = [slice(k, k + 128) for k in range(0, chunk, 128)]
        m_old = m_s[...]
        m_new = m_old
        for p in parts:
            m_new = jnp.maximum(m_new, z[:, p])
        base = jnp.where(m_new == -jnp.inf, 0.0, m_new)
        s = s_s[...] * jnp.exp(m_old - base)
        ts = ts_s[...]
        tzs = tz_s[...]
        for p in parts:
            s += jnp.exp(z[:, p] - base)
            ts += t[:, p]
            tzs += tz[:, p]
        m_s[...] = m_new
        s_s[...] = s
        ts_s[...] = ts
        tz_s[...] = tzs
        return carry

    lax.fori_loop(0, n_chunks, logits, 0)

    m = m_s[...].max(axis=1, keepdims=True)
    s = (s_s[...] * jnp.exp(m_s[...] - m)).sum(axis=1, keepdims=True)
    ts = ts_s[...].sum(axis=1, keepdims=True)
    tz = tz_s[...].sum(axis=1, keepdims=True)
    lane = lax.broadcasted_iota(jnp.int32, m_s.shape, 1)
    packed = jnp.where(lane == 0, m, jnp.where(lane == 1, s, jnp.where(lane == 2, ts, tz)))
    stat_s[vp] = packed.T[:8]

    pl.semaphore_wait(barrier, vp_size + 2)
    copies = []
    for k, o in enumerate(others):
        c = pltpu.make_async_remote_copy(
            src_ref=stat_s.at[vp], dst_ref=stat_s.at[vp], send_sem=stat_send.at[k], recv_sem=stat_recv.at[k],
            device_id=(o, dp), device_id_type=MESH,
        )
        c.start()
        copies.append(c)
    ut_s[...] = u_ref[...].T
    for c in copies:
        c.wait()

    stat = [stat_s[k] for k in range(vp_size)]
    m = functools.reduce(jnp.maximum, [a[0:1] for a in stat])
    s = sum(a[1:2] * jnp.exp(a[0:1] - m) for a in stat)
    ts = sum(a[2:3] for a in stat)
    tz = sum(a[3:4] for a in stat)
    log_norm = m + jnp.log(s)
    loss = (log_norm * ts - tz).sum(axis=1, keepdims=True)
    row = lax.broadcasted_iota(jnp.int32, (128, m.shape[1]), 0)
    col_s[...] = jnp.where(row == 0, log_norm, ts).T

    def grads(i, carry):
        cols = pl.ds(pl.multiple_of(i * chunk, chunk), chunk)
        g = (jnp.exp(z_s[:images, cols] - col_s[:, 0:1]) * col_s[:, 1:2] - t_s[:images, cols]) * (1.0 / n_glob)
        g_s[:, cols] = g.astype(BF16)
        db_s[0, :, cols] = g.sum(axis=0, keepdims=True)
        return carry

    lax.fori_loop(0, n_chunks, grads, 0)
    db_s[0, :, classes:] = loss + jnp.zeros((1, padded - classes), F32)

    pl.semaphore_signal(ready_sem, inc=1, device_id=(vp, sib), device_id_type=MESH)

    def db_copy(k, who):
        return pltpu.make_async_remote_copy(
            src_ref=db_s.at[2 * k], dst_ref=db_s.at[2 * k + 1], send_sem=db_send.at[k], recv_sem=db_recv.at[k],
            device_id=(vp, who), device_id_type=MESH,
        )

    db_copies = [db_copy(0, sib), db_copy(1, along_x), db_copy(2, along_y)]

    def db_next(k):
        db_copies[k].wait()
        if k < 2:
            db_s[2 * k + 2] = db_s[2 * k] + db_s[2 * k + 1]
            db_copies[k + 1].start()
        else:
            db_ref[...] = db_s[4] + db_s[5]

    db_copies[0].start()

    def dots(src, n, dst, add):
        left = ut_s[pl.ds(pl.multiple_of(src * part, part), n), :]

        def body(i, carry):
            cols = pl.ds(pl.multiple_of(i * chunk, chunk), chunk)
            v = jnp.dot(left, g_s[:, cols], preferred_element_type=F32)
            at = pl.ds(dst, n)
            if add:
                t_s[at, cols] = t_s[at, cols] + v
            else:
                z_s[at, cols] = v
            return carry

        lax.fori_loop(0, n_chunks, body, 0)

    def to_sibling(k, at):
        rows = pl.ds(pl.multiple_of(at * part, part), part)
        return pltpu.make_async_remote_copy(
            src_ref=z_s.at[rows, pl.ds(0, classes)], dst_ref=t_s.at[pl.ds(k * part, part), pl.ds(0, classes)],
            send_sem=sib_send.at[k], recv_sem=sib_recv.at[k], device_id=(vp, sib), device_id_type=MESH,
        )

    dots(4 * (1 - core) + 2 * (1 - p2), 2 * part, 0, False)
    sends = [to_sibling(0, 1 - p1), to_sibling(1, p1), to_sibling(2, 3 - p1), to_sibling(3, 2 + p1)]
    pl.semaphore_wait(ready_sem, 1)
    sends[0].start()
    db_next(0)
    dots(4 * (1 - core) + 2 * p2, 2 * part, 2 * part, False)
    sends[1].start()
    db_next(1)

    own = [4 * core + 2 * a + b for a, b in ((1 - p1, 1 - p2), (1 - p1, p2), (p1, 1 - p2), (p1, p2))]

    def piece(k):
        return t_s.at[pl.ds(k * part, part), pl.ds(0, classes)]

    sends[0].wait_recv()
    sends[2].start()
    sends[3].start()
    dots(own[0], part, 0, True)
    far = pltpu.make_async_remote_copy(
        src_ref=piece(0), dst_ref=ra_s, send_sem=far_sem.at[0], recv_sem=far_sem.at[1],
        device_id=(vp, first), device_id_type=MESH,
    )
    far.start()

    def du_dot(i, carry):
        cols = pl.ds(pl.multiple_of(i * chunk, chunk), chunk)
        v = lax.dot_general(g_s[:, cols], w_s[:, cols], (((1,), (1,)), ((), ())), preferred_element_type=F32)
        du_s[...] = du_s[...] + v
        return carry

    du_s[...] = jnp.zeros_like(du_s)
    lax.fori_loop(0, n_chunks, du_dot, 0)
    keep = pl.ds(pl.multiple_of(z0 * half, half), half)
    give = pl.ds(pl.multiple_of((1 - z0) * half, half), half)
    du_copy = pltpu.make_async_remote_copy(
        src_ref=du_s.at[give], dst_ref=du_in, send_sem=du_sem.at[0], recv_sem=du_sem.at[1],
        device_id=(near, dp), device_id_type=MESH,
    )
    du_copy.start()
    db_next(2)

    outs = []
    for k, out in ((1, pb_hbm), (2, pc_hbm), (3, pd_hbm)):
        sends[k].wait_recv()
        dots(own[k], part, k * part, True)
        c = pltpu.make_async_copy(piece(k), out, out_sem.at[k - 1])
        if k != 2:
            c.start()
        outs.append(c)
    for c in sends:
        c.wait_send()
    du_copy.wait()
    du_ref[...] = du_s[keep, :] + du_in[...]
    far.wait()

    def add_far(i, carry):
        cols = pl.ds(pl.multiple_of(i * 128, 128), 128)
        at = pl.ds(2 * part, part)
        t_s[at, cols] = t_s[at, cols] + ra_s[:, cols]
        return carry

    lax.fori_loop(0, classes // 128, add_far, 0)
    outs[1].start()
    for c in outs:
        c.wait()


def head(u, b, w, t, n_glob, vp_size):
    images, width = u.shape
    classes = w.shape[1]
    padded = (classes // 512 + 1) * 512
    part = width // 8
    rows = max(images, 4 * part)
    any_spec = pl.BlockSpec(memory_space=pl.ANY)
    vmem = pl.BlockSpec(memory_space=pltpu.VMEM)
    dma = pltpu.SemaphoreType.DMA
    piece = jax.ShapeDtypeStruct((part, classes), F32)
    return pl.pallas_call(
        functools.partial(head_kernel, n_glob),
        in_specs=[vmem, vmem, any_spec, any_spec],
        out_specs=[any_spec] * 3 + [vmem] * 2,
        out_shape=[piece] * 3 + [
            jax.ShapeDtypeStruct((images // 2, width), F32),
            jax.ShapeDtypeStruct((1, padded), F32),
        ],
        scratch_shapes=[
            pltpu.VMEM((width, padded), BF16),
            pltpu.VMEM((rows, padded), F32),
            pltpu.VMEM((rows, padded), F32),
            pltpu.VMEM((part, classes), F32),
            pltpu.VMEM((1, padded), F32),
            pltpu.VMEM((6, 1, padded), F32),
            pltpu.VMEM((images, padded), BF16),
            pltpu.VMEM((width, images), BF16),
        ] + [pltpu.VMEM((images, 128), F32)] * 4 + [
            pltpu.VMEM((vp_size, 8, images), F32),
            pltpu.VMEM((images, 128), F32),
            pltpu.VMEM((images, width), F32),
            pltpu.VMEM((images // 2, width), F32),
            dma((2, padded // 512)),
            dma((vp_size - 1,)),
            dma((vp_size - 1,)),
            dma((4,)),
            dma((4,)),
            dma((2,)),
            dma((2,)),
            dma((3,)),
            dma((3,)),
            dma((3,)),
            pltpu.SemaphoreType.REGULAR,
        ],
        compiler_params=pltpu.CompilerParams(
            collective_id=0, has_side_effects=True, vmem_limit_bytes=60 * 1024 * 1024
        ),
        cost_estimate=pl.CostEstimate(
            flops=6 * images * width * classes, bytes_accessed=20 * width * classes, transcendentals=0
        ),
        name="head",
    )(u, b[None], w, t)


def solution(mesh):
    dp_size = mesh.shape["dp"]
    vp_size = mesh.shape["vp"]
    sibling = [(i, i ^ 1) for i in range(8)]
    first = [(i, i ^ (4 if i & 1 else 2)) for i in range(8)]
    second = [(i, i ^ (2 if i & 1 else 4)) for i in range(8)]
    near = [(i, i ^ 1) for i in range(vp_size)]
    distant = [(i, i ^ 2) for i in range(vp_size)]

    def local_step(h_loc, gamma, beta, w_loc, b_loc, t_loc):
        images, _, width = h_loc.shape
        n_glob = images * dp_size
        classes = w_loc.shape[1]
        part = width // 8
        quarter = images // 4
        dp = lax.axis_index("dp")
        vp = lax.axis_index("vp")
        core, x, y = dp & 1, (dp >> 1) & 1, dp >> 2
        z0, z1 = vp & 1, vp >> 1
        p1 = jnp.where(core == 0, x, y)
        p2 = jnp.where(core == 0, y, x)
        own = [4 * core + 2 * a + b for a, b in ((1 - p1, 1 - p2), (1 - p1, p2), (p1, 1 - p2), (p1, p2))]
        sib = [4 * (1 - core) + 2 * a + b for a, b in ((1 - p2, 1 - p1), (1 - p2, p1), (p2, 1 - p1), (p2, p1))]

        ht = h_loc.transpose(1, 0, 2)
        u = pool_forward(ht, gamma, beta)
        b, c, d, du_half, db = head(u, b_loc, w_loc, t_loc, n_glob, vp_size)

        def send(v, pairs):
            return lax.ppermute(v, "dp", pairs)

        r_d = send(b, first)
        r_d2 = send(c, second)

        got = lax.ppermute(lax.dynamic_slice(du_half, ((1 - z1) * quarter, 0), (quarter, width)), "vp", distant)
        du_own = lax.dynamic_slice(du_half, (z1 * quarter, 0), (quarter, width)) + got
        du_far = lax.ppermute(du_own, "vp", distant)
        du_near = lax.ppermute(du_own, "vp", near)
        du_last = lax.ppermute(du_far, "vp", near)

        dh, token = pool_backward(ht, du_own, gamma, None, 2 * z0 + z1, du_own)
        dh, token = pool_backward(ht, du_far, gamma, dh, 2 * z0 + 1 - z1, token)
        d = ((d + r_d) + r_d2) + token[0, 0]
        c_fin = send(d, second)
        b_fin = send(d, first)
        dh, token = pool_backward(ht, du_near, gamma, dh, 2 * (1 - z0) + z1, d)
        dh, token = pool_backward(ht, du_last, gamma, dh, 2 * (1 - z0) + 1 - z1, token)
        a_fin = send(c_fin, first)
        mine = [a_fin, b_fin, c_fin, d]
        theirs = [send(v, sibling) for v in mine]

        out = place_first(d, own[3], width)
        for v, k in ((theirs[3], sib[3]), (mine[2], own[2]), (theirs[2], sib[2]),
                     (mine[1], own[1]), (theirs[1], sib[1]), (mine[0], own[0]), (theirs[0], sib[0])):
            out = lax.dynamic_update_slice(out, v, (k * part, 0))
        return db[0, classes] / n_glob, out, db[0, :classes], dh.transpose(1, 0, 2)

    return jax.shard_map(
        local_step,
        mesh=mesh,
        in_specs=(P("dp", None, None), P(), P(), P(None, "vp"), P("vp"), P("dp", "vp")),
        out_specs=(P(), P(None, "vp"), P("vp"), P("dp", None, None)),
        check_vma=False,
    )
```

```python
import functools

import jax
import jax.numpy as jnp
from jax import lax
from jax.experimental import pallas as pl
from jax.experimental.pallas import tpu as pltpu
from jax.sharding import PartitionSpec as P


NUM_CLASSES = 21841
LN_EPS = 1e-5
F32 = jnp.float32
BF16 = jnp.bfloat16
MESH = pl.DeviceIdType.MESH


def norm_rows(x):
    width = x.shape[-1]
    c = x - x.sum(axis=-1, keepdims=True) * (1.0 / width)
    var = (c * c).sum(axis=-1, keepdims=True) * (1.0 / width)
    return c, lax.rsqrt(var + LN_EPS)


def pool_kernel(h_ref, gamma_ref, beta_ref, u_ref, acc_ref):
    tokens, rows, _ = h_ref.shape
    acc_ref[...] = jnp.zeros_like(acc_ref)

    def group(i, carry):
        here = pl.ds(pl.multiple_of(i * 16, 16), 16)
        for t in range(tokens):
            c, r = norm_rows(h_ref[t, here, :].astype(F32))
            acc_ref[here, :] += c * r
        return carry

    lax.fori_loop(0, rows // 16, group, 0)
    u = acc_ref[...] * (gamma_ref[...] * (1.0 / tokens)) + beta_ref[...]
    u_ref[...] = u.astype(BF16)


def pool_forward(ht, gamma, beta, rows=32):
    tokens, images, width = ht.shape
    rows = min(rows, images)
    return pl.pallas_call(
        pool_kernel,
        grid=(images // rows,),
        in_specs=[
            pl.BlockSpec((tokens, rows, width), lambda i: (0, i, 0)),
            pl.BlockSpec((1, width), lambda i: (0, 0)),
            pl.BlockSpec((1, width), lambda i: (0, 0)),
        ],
        out_specs=pl.BlockSpec((rows, width), lambda i: (i, 0)),
        out_shape=jax.ShapeDtypeStruct((images, width), BF16),
        scratch_shapes=[pltpu.VMEM((rows, width), F32)],
        compiler_params=pltpu.CompilerParams(dimension_semantics=("arbitrary",)),
        cost_estimate=pl.CostEstimate(flops=8 * ht.size * 40, bytes_accessed=2 * ht.size, transcendentals=0),
        name="pool_forward",
    )(ht, gamma[None], beta[None])


def pool_backward_kernel(off_ref, h_ref, du_ref, gamma_ref, *rest):
    dh_ref, token_ref, v_ref = rest[-3:]
    tokens, rows, width = h_ref.shape
    v = du_ref[...] * (gamma_ref[...] * (1.0 / tokens))
    v_ref[...] = v - v.sum(axis=-1, keepdims=True) * (1.0 / width)
    token_ref[...] = jnp.zeros_like(token_ref)

    def group(i, carry):
        here = pl.ds(pl.multiple_of(i * 16, 16), 16)
        for t in range(tokens):
            c, r = norm_rows(h_ref[t, here, :].astype(F32))
            vc = v_ref[here, :]
            xhat = c * r
            k = (vc * xhat).sum(axis=-1, keepdims=True) * (1.0 / width)
            dh_ref[t, here, :] = ((vc - xhat * k) * r).astype(BF16)
        return carry

    lax.fori_loop(0, rows // 16, group, 0)


def pool_backward(ht, du, gamma, buf, block, after, rows=32):
    tokens, images, width = ht.shape
    count = du.shape[0]
    rows = min(rows, count)
    steps = count // rows
    any_spec = pl.BlockSpec(memory_space=pl.ANY)
    in_specs = [
        pl.BlockSpec((tokens, rows, width), lambda i, o: (0, o[0] + i, 0)),
        pl.BlockSpec((rows, width), lambda i, o: (i, 0)),
        pl.BlockSpec((1, width), lambda i, o: (0, 0)),
        any_spec,
    ]
    args = [(block * steps).astype(jnp.int32)[None], ht, du, gamma[None], after]
    aliases = {}
    if buf is not None:
        in_specs.append(any_spec)
        args.append(buf)
        aliases = {5: 0}
    return pl.pallas_call(
        pool_backward_kernel,
        grid_spec=pltpu.PrefetchScalarGridSpec(
            num_scalar_prefetch=1,
            grid=(steps,),
            in_specs=in_specs,
            out_specs=[
                pl.BlockSpec((tokens, rows, width), lambda i, o: (0, o[0] + i, 0)),
                pl.BlockSpec((8, 128), lambda i, o: (0, 0)),
            ],
            scratch_shapes=[pltpu.VMEM((rows, width), F32)],
        ),
        out_shape=[
            jax.ShapeDtypeStruct((tokens, images, width), BF16),
            jax.ShapeDtypeStruct((8, 128), F32),
        ],
        input_output_aliases=aliases,
        compiler_params=pltpu.CompilerParams(dimension_semantics=("arbitrary",)),
        cost_estimate=pl.CostEstimate(
            flops=40 * 12 * tokens * count * width, bytes_accessed=4 * tokens * count * width, transcendentals=0
        ),
        name="pool_backward",
    )(*args)


def place_kernel(off_ref, v_ref, o_ref):
    o_ref[...] = v_ref[...]


def place_first(v, block, total_rows, rows=32):
    count, n = v.shape
    steps = count // rows
    return pl.pallas_call(
        place_kernel,
        grid_spec=pltpu.PrefetchScalarGridSpec(
            num_scalar_prefetch=1,
            grid=(steps,),
            in_specs=[pl.BlockSpec((rows, n), lambda i, o: (i, 0))],
            out_specs=pl.BlockSpec((rows, n), lambda i, o: (o[0] + i, 0)),
        ),
        out_shape=jax.ShapeDtypeStruct((total_rows, n), v.dtype),
        cost_estimate=pl.CostEstimate(flops=10 * v.size, bytes_accessed=8 * v.size, transcendentals=0),
        name="place_first",
    )((block * steps).astype(jnp.int32)[None], v)


def head_kernel(
    n_glob, u_ref, b_ref, w_hbm, t_hbm,
    pb_hbm, pc_hbm, pd_hbm, du_ref, db_ref,
    w_s, t_s, z_s, ra_s, b_s, db_s, g_s, ut_s, m_s, s_s, ts_s, tz_s, stat_s, col_s, du_s, du_in,
    load_sem, stat_send, stat_recv, sib_send, sib_recv, far_sem, du_sem, db_send, db_recv, out_sem, ready_sem,
):
    images, width = u_ref.shape
    classes = w_hbm.shape[1]
    padded = w_s.shape[1]
    chunk = 512
    n_chunks = padded // chunk
    tail = classes - (n_chunks - 1) * chunk
    part = width // 8
    half = images // 2

    vp = lax.axis_index("vp")
    dp = lax.axis_index("dp")
    core, x, y = lax.rem(dp, 2), lax.rem(dp // 2, 2), dp // 4
    p1 = jnp.where(core == 0, x, y)
    p2 = jnp.where(core == 0, y, x)
    sib = dp + 1 - 2 * core
    along_x, along_y = dp + 2 - 4 * x, dp + 4 - 8 * y
    first = jnp.where(core == 0, along_x, along_y)
    z0 = lax.rem(vp, 2)
    near = vp + 1 - 2 * z0
    vp_size = stat_s.shape[0]
    others = [lax.rem(vp + k, vp_size) for k in range(1, vp_size)]

    barrier = pltpu.get_barrier_semaphore()
    for who in [(o, dp) for o in others] + [(vp, sib), (vp, along_x), (vp, along_y)]:
        pl.semaphore_signal(barrier, inc=1, device_id=who, device_id_type=MESH)

    def loads(i, n):
        cols = pl.ds(pl.multiple_of(i * chunk, chunk), n)
        return (
            pltpu.make_async_copy(w_hbm.at[:, cols], w_s.at[:, cols], load_sem.at[0, i]),
            pltpu.make_async_copy(t_hbm.at[:, cols], t_s.at[pl.ds(0, images), cols], load_sem.at[1, i]),
        )

    ahead = min(4, n_chunks - 1)
    for i in range(ahead):
        for c in loads(i, chunk):
            c.start()
    if padded > classes:
        b_s[:, classes:] = jnp.zeros((1, padded - classes), F32)
        w_s[:, classes:] = jnp.zeros((width, padded - classes), BF16)
        t_s[:, classes:] = jnp.zeros((t_s.shape[0], padded - classes), F32)
    b_s[:, :classes] = b_ref[...]
    m_s[...] = jnp.full_like(m_s, -jnp.inf)
    s_s[...] = jnp.zeros_like(s_s)
    ts_s[...] = jnp.zeros_like(ts_s)
    tz_s[...] = jnp.zeros_like(tz_s)
    limit = jnp.minimum(classes, NUM_CLASSES - vp * classes)

    def logits(i, carry):
        @pl.when(i + ahead < n_chunks - 1)
        def _():
            for c in loads(i + ahead, chunk):
                c.start()

        @pl.when(i + ahead == n_chunks - 1)
        def _():
            for c in loads(n_chunks - 1, tail):
                c.start()

        @pl.when(i < n_chunks - 1)
        def _():
            for c in loads(i, chunk):
                c.wait()

        @pl.when(i == n_chunks - 1)
        def _():
            for c in loads(n_chunks - 1, tail):
                c.wait()

        cols = pl.ds(pl.multiple_of(i * chunk, chunk), chunk)
        z = jnp.dot(u_ref[...], w_s[:, cols], preferred_element_type=F32) + b_s[:, cols]
        valid = i * chunk + lax.broadcasted_iota(jnp.int32, (1, chunk), 1) < limit
        t = t_s[:images, cols]
        tz = t * jnp.where(valid, z, 0.0)
        z = jnp.where(valid, z, -jnp.inf)
        z_s[:images, cols] = z
        parts = [slice(k, k + 128) for k in range(0, chunk, 128)]
        m_old = m_s[...]
        m_new = m_old
        for p in parts:
            m_new = jnp.maximum(m_new, z[:, p])
        base = jnp.where(m_new == -jnp.inf, 0.0, m_new)
        s = s_s[...] * jnp.exp(m_old - base)
        ts = ts_s[...]
        tzs = tz_s[...]
        for p in parts:
            s += jnp.exp(z[:, p] - base)
            ts += t[:, p]
            tzs += tz[:, p]
        m_s[...] = m_new
        s_s[...] = s
        ts_s[...] = ts
        tz_s[...] = tzs
        return carry

    lax.fori_loop(0, n_chunks, logits, 0)

    m = m_s[...].max(axis=1, keepdims=True)
    s = (s_s[...] * jnp.exp(m_s[...] - m)).sum(axis=1, keepdims=True)
    ts = ts_s[...].sum(axis=1, keepdims=True)
    tz = tz_s[...].sum(axis=1, keepdims=True)
    lane = lax.broadcasted_iota(jnp.int32, m_s.shape, 1)
    packed = jnp.where(lane == 0, m, jnp.where(lane == 1, s, jnp.where(lane == 2, ts, tz)))
    stat_s[vp] = packed.T[:8]

    pl.semaphore_wait(barrier, vp_size + 2)
    copies = []
    for k, o in enumerate(others):
        c = pltpu.make_async_remote_copy(
            src_ref=stat_s.at[vp], dst_ref=stat_s.at[vp], send_sem=stat_send.at[k], recv_sem=stat_recv.at[k],
            device_id=(o, dp), device_id_type=MESH,
        )
        c.start()
        copies.append(c)
    ut_s[...] = u_ref[...].T
    for c in copies:
        c.wait()

    stat = [stat_s[k] for k in range(vp_size)]
    m = functools.reduce(jnp.maximum, [a[0:1] for a in stat])
    s = sum(a[1:2] * jnp.exp(a[0:1] - m) for a in stat)
    ts = sum(a[2:3] for a in stat)
    tz = sum(a[3:4] for a in stat)
    log_norm = m + jnp.log(s)
    loss = (log_norm * ts - tz).sum(axis=1, keepdims=True)
    row = lax.broadcasted_iota(jnp.int32, (128, m.shape[1]), 0)
    col_s[...] = jnp.where(row == 0, log_norm, ts).T

    def grads(i, carry):
        cols = pl.ds(pl.multiple_of(i * chunk, chunk), chunk)
        g = (jnp.exp(z_s[:images, cols] - col_s[:, 0:1]) * col_s[:, 1:2] - t_s[:images, cols]) * (1.0 / n_glob)
        g_s[:, cols] = g.astype(BF16)
        db_s[0, :, cols] = g.sum(axis=0, keepdims=True)
        return carry

    lax.fori_loop(0, n_chunks, grads, 0)
    db_s[0, :, classes:] = loss + jnp.zeros((1, padded - classes), F32)

    pl.semaphore_signal(ready_sem, inc=1, device_id=(vp, sib), device_id_type=MESH)

    def db_copy(k, who):
        return pltpu.make_async_remote_copy(
            src_ref=db_s.at[2 * k], dst_ref=db_s.at[2 * k + 1], send_sem=db_send.at[k], recv_sem=db_recv.at[k],
            device_id=(vp, who), device_id_type=MESH,
        )

    db_copies = [db_copy(0, sib), db_copy(1, along_x), db_copy(2, along_y)]

    def db_next(k):
        db_copies[k].wait()
        if k < 2:
            db_s[2 * k + 2] = db_s[2 * k] + db_s[2 * k + 1]
            db_copies[k + 1].start()
        else:
            db_ref[...] = db_s[4] + db_s[5]

    db_copies[0].start()

    def dots(src, n, dst, add):
        left = ut_s[pl.ds(pl.multiple_of(src * part, part), n), :]

        def body(i, carry):
            cols = pl.ds(pl.multiple_of(i * chunk, chunk), chunk)
            v = jnp.dot(left, g_s[:, cols], preferred_element_type=F32)
            at = pl.ds(dst, n)
            if add:
                t_s[at, cols] = t_s[at, cols] + v
            else:
                z_s[at, cols] = v
            return carry

        lax.fori_loop(0, n_chunks, body, 0)

    def to_sibling(k, at):
        rows = pl.ds(pl.multiple_of(at * part, part), part)
        return pltpu.make_async_remote_copy(
            src_ref=z_s.at[rows, pl.ds(0, classes)], dst_ref=t_s.at[pl.ds(k * part, part), pl.ds(0, classes)],
            send_sem=sib_send.at[k], recv_sem=sib_recv.at[k], device_id=(vp, sib), device_id_type=MESH,
        )

    dots(4 * (1 - core) + 2 * (1 - p2), 2 * part, 0, False)
    sends = [to_sibling(0, 1 - p1), to_sibling(1, p1), to_sibling(2, 3 - p1), to_sibling(3, 2 + p1)]
    pl.semaphore_wait(ready_sem, 1)
    sends[0].start()
    db_next(0)
    dots(4 * (1 - core) + 2 * p2, 2 * part, 2 * part, False)
    sends[1].start()
    db_next(1)

    own = [4 * core + 2 * a + b for a, b in ((1 - p1, 1 - p2), (1 - p1, p2), (p1, 1 - p2), (p1, p2))]

    def piece(k):
        return t_s.at[pl.ds(k * part, part), pl.ds(0, classes)]

    sends[0].wait_recv()
    sends[2].start()
    sends[3].start()
    dots(own[0], part, 0, True)
    far = pltpu.make_async_remote_copy(
        src_ref=piece(0), dst_ref=ra_s, send_sem=far_sem.at[0], recv_sem=far_sem.at[1],
        device_id=(vp, first), device_id_type=MESH,
    )
    far.start()

    def du_dot(i, carry):
        cols = pl.ds(pl.multiple_of(i * chunk, chunk), chunk)
        v = lax.dot_general(g_s[:, cols], w_s[:, cols], (((1,), (1,)), ((), ())), preferred_element_type=F32)
        du_s[...] = du_s[...] + v
        return carry

    du_s[...] = jnp.zeros_like(du_s)
    lax.fori_loop(0, n_chunks, du_dot, 0)
    keep = pl.ds(pl.multiple_of(z0 * half, half), half)
    give = pl.ds(pl.multiple_of((1 - z0) * half, half), half)
    du_copy = pltpu.make_async_remote_copy(
        src_ref=du_s.at[give], dst_ref=du_in, send_sem=du_sem.at[0], recv_sem=du_sem.at[1],
        device_id=(near, dp), device_id_type=MESH,
    )
    du_copy.start()
    db_next(2)

    outs = []
    for k, out in ((1, pb_hbm), (2, pc_hbm), (3, pd_hbm)):
        sends[k].wait_recv()
        dots(own[k], part, k * part, True)
        c = pltpu.make_async_copy(piece(k), out, out_sem.at[k - 1])
        if k != 2:
            c.start()
        outs.append(c)
    for c in sends:
        c.wait_send()
    du_copy.wait()
    du_ref[...] = du_s[keep, :] + du_in[...]
    far.wait()

    def add_far(i, carry):
        cols = pl.ds(pl.multiple_of(i * 128, 128), 128)
        at = pl.ds(2 * part, part)
        t_s[at, cols] = t_s[at, cols] + ra_s[:, cols]
        return carry

    lax.fori_loop(0, classes // 128, add_far, 0)
    outs[1].start()
    for c in outs:
        c.wait()


def head(u, b, w, t, n_glob, vp_size):
    images, width = u.shape
    classes = w.shape[1]
    padded = (classes // 512 + 1) * 512
    part = width // 8
    rows = max(images, 4 * part)
    any_spec = pl.BlockSpec(memory_space=pl.ANY)
    vmem = pl.BlockSpec(memory_space=pltpu.VMEM)
    dma = pltpu.SemaphoreType.DMA
    piece = jax.ShapeDtypeStruct((part, classes), F32)
    return pl.pallas_call(
        functools.partial(head_kernel, n_glob),
        in_specs=[vmem, vmem, any_spec, any_spec],
        out_specs=[any_spec] * 3 + [vmem] * 2,
        out_shape=[piece] * 3 + [
            jax.ShapeDtypeStruct((images // 2, width), F32),
            jax.ShapeDtypeStruct((1, padded), F32),
        ],
        scratch_shapes=[
            pltpu.VMEM((width, padded), BF16),
            pltpu.VMEM((rows, padded), F32),
            pltpu.VMEM((rows, padded), F32),
            pltpu.VMEM((part, classes), F32),
            pltpu.VMEM((1, padded), F32),
            pltpu.VMEM((6, 1, padded), F32),
            pltpu.VMEM((images, padded), BF16),
            pltpu.VMEM((width, images), BF16),
        ] + [pltpu.VMEM((images, 128), F32)] * 4 + [
            pltpu.VMEM((vp_size, 8, images), F32),
            pltpu.VMEM((images, 128), F32),
            pltpu.VMEM((images, width), F32),
            pltpu.VMEM((images // 2, width), F32),
            dma((2, padded // 512)),
            dma((vp_size - 1,)),
            dma((vp_size - 1,)),
            dma((4,)),
            dma((4,)),
            dma((2,)),
            dma((2,)),
            dma((3,)),
            dma((3,)),
            dma((3,)),
            pltpu.SemaphoreType.REGULAR,
        ],
        compiler_params=pltpu.CompilerParams(
            collective_id=0, has_side_effects=True, vmem_limit_bytes=60 * 1024 * 1024
        ),
        cost_estimate=pl.CostEstimate(
            flops=6 * images * width * classes, bytes_accessed=20 * width * classes, transcendentals=0
        ),
        name="head",
    )(u, b[None], w, t)


def solution(mesh):
    dp_size = mesh.shape["dp"]
    vp_size = mesh.shape["vp"]
    sibling = [(i, i ^ 1) for i in range(8)]
    first = [(i, i ^ (4 if i & 1 else 2)) for i in range(8)]
    second = [(i, i ^ (2 if i & 1 else 4)) for i in range(8)]
    near = [(i, i ^ 1) for i in range(vp_size)]
    distant = [(i, i ^ 2) for i in range(vp_size)]

    def local_step(h_loc, gamma, beta, w_loc, b_loc, t_loc):
        images, _, width = h_loc.shape
        n_glob = images * dp_size
        classes = w_loc.shape[1]
        part = width // 8
        quarter = images // 4
        dp = lax.axis_index("dp")
        vp = lax.axis_index("vp")
        core, x, y = dp & 1, (dp >> 1) & 1, dp >> 2
        z0, z1 = vp & 1, vp >> 1
        p1 = jnp.where(core == 0, x, y)
        p2 = jnp.where(core == 0, y, x)
        own = [4 * core + 2 * a + b for a, b in ((1 - p1, 1 - p2), (1 - p1, p2), (p1, 1 - p2), (p1, p2))]
        sib = [4 * (1 - core) + 2 * a + b for a, b in ((1 - p2, 1 - p1), (1 - p2, p1), (p2, 1 - p1), (p2, p1))]

        ht = h_loc.transpose(1, 0, 2)
        u = pool_forward(ht, gamma, beta)
        b, c, d, du_half, db = head(u, b_loc, w_loc, t_loc, n_glob, vp_size)

        def send(v, pairs):
            return lax.ppermute(v, "dp", pairs)

        r_d = send(b, first)
        r_d2 = send(c, second)

        got = lax.ppermute(lax.dynamic_slice(du_half, ((1 - z1) * quarter, 0), (quarter, width)), "vp", distant)
        du_own = lax.dynamic_slice(du_half, (z1 * quarter, 0), (quarter, width)) + got
        du_far = lax.ppermute(du_own, "vp", distant)
        du_near = lax.ppermute(du_own, "vp", near)
        du_last = lax.ppermute(du_far, "vp", near)

        dh, token = pool_backward(ht, du_own, gamma, None, 2 * z0 + z1, du_own)
        d = ((d + r_d) + r_d2) + token[0, 0]
        c_fin = send(d, second)
        b_fin = send(d, first)
        dh, token = pool_backward(ht, du_far, gamma, dh, 2 * z0 + 1 - z1, d)
        dh, token = pool_backward(ht, du_near, gamma, dh, 2 * (1 - z0) + z1, token)
        dh, token = pool_backward(ht, du_last, gamma, dh, 2 * (1 - z0) + 1 - z1, token)
        a_fin = send(c_fin, first)
        mine = [a_fin, b_fin, c_fin, d]
        theirs = [send(v, sibling) for v in mine]

        out = place_first(d, own[3], width)
        for v, k in ((theirs[3], sib[3]), (mine[2], own[2]), (theirs[2], sib[2]),
                     (mine[1], own[1]), (theirs[1], sib[1]), (mine[0], own[0]), (theirs[0], sib[0])):
            out = lax.dynamic_update_slice(out, v, (k * part, 0))
        loss, db = db[0, classes] / n_glob, db[0, :classes]
        return loss, out, db, dh.transpose(1, 0, 2)

    return jax.shard_map(
        local_step,
        mesh=mesh,
        in_specs=(P("dp", None, None), P(), P(), P(None, "vp"), P("vp"), P("dp", "vp")),
        out_specs=(P(), P(None, "vp"), P("vp"), P("dp", None, None)),
        check_vma=False,
    )
```

```python
import functools

import jax
import jax.numpy as jnp
from jax import lax
from jax.experimental import pallas as pl
from jax.experimental.pallas import tpu as pltpu
from jax.sharding import PartitionSpec as P


NUM_CLASSES = 21841
LN_EPS = 1e-5
F32 = jnp.float32
BF16 = jnp.bfloat16
MESH = pl.DeviceIdType.MESH


def norm_rows(x):
    width = x.shape[-1]
    c = x - x.sum(axis=-1, keepdims=True) * (1.0 / width)
    var = (c * c).sum(axis=-1, keepdims=True) * (1.0 / width)
    return c, lax.rsqrt(var + LN_EPS)


def pool_backward_kernel(off_ref, h_ref, du_ref, gamma_ref, *rest):
    dh_ref, token_ref, v_ref = rest[-3:]
    tokens, rows, width = h_ref.shape
    v = du_ref[...] * (gamma_ref[...] * (1.0 / tokens))
    v_ref[...] = v - v.sum(axis=-1, keepdims=True) * (1.0 / width)
    token_ref[...] = jnp.zeros_like(token_ref)

    def group(i, carry):
        here = pl.ds(pl.multiple_of(i * 16, 16), 16)
        for t in range(tokens):
            c, r = norm_rows(h_ref[t, here, :].astype(F32))
            vc = v_ref[here, :]
            xhat = c * r
            k = (vc * xhat).sum(axis=-1, keepdims=True) * (1.0 / width)
            dh_ref[t, here, :] = ((vc - xhat * k) * r).astype(BF16)
        return carry

    lax.fori_loop(0, rows // 16, group, 0)


def pool_backward(ht, du, gamma, buf, block, after, rows=32):
    tokens, images, width = ht.shape
    count = du.shape[0]
    rows = min(rows, count)
    steps = count // rows
    any_spec = pl.BlockSpec(memory_space=pl.ANY)
    in_specs = [
        pl.BlockSpec((tokens, rows, width), lambda i, o: (0, o[0] + i, 0)),
        pl.BlockSpec((rows, width), lambda i, o: (i, 0)),
        pl.BlockSpec((1, width), lambda i, o: (0, 0)),
        any_spec,
    ]
    args = [(block * steps).astype(jnp.int32)[None], ht, du, gamma[None], after]
    aliases = {}
    if buf is not None:
        in_specs.append(any_spec)
        args.append(buf)
        aliases = {5: 0}
    return pl.pallas_call(
        pool_backward_kernel,
        grid_spec=pltpu.PrefetchScalarGridSpec(
            num_scalar_prefetch=1,
            grid=(steps,),
            in_specs=in_specs,
            out_specs=[
                pl.BlockSpec((tokens, rows, width), lambda i, o: (0, o[0] + i, 0)),
                pl.BlockSpec((8, 128), lambda i, o: (0, 0)),
            ],
            scratch_shapes=[pltpu.VMEM((rows, width), F32)],
        ),
        out_shape=[
            jax.ShapeDtypeStruct((tokens, images, width), BF16),
            jax.ShapeDtypeStruct((8, 128), F32),
        ],
        input_output_aliases=aliases,
        compiler_params=pltpu.CompilerParams(dimension_semantics=("arbitrary",)),
        cost_estimate=pl.CostEstimate(
            flops=40 * 12 * tokens * count * width, bytes_accessed=4 * tokens * count * width, transcendentals=0
        ),
        name="pool_backward",
    )(*args)


def place_kernel(off_ref, v_ref, o_ref):
    o_ref[...] = v_ref[...]


def place_first(v, block, total_rows, rows=32):
    count, n = v.shape
    steps = count // rows
    return pl.pallas_call(
        place_kernel,
        grid_spec=pltpu.PrefetchScalarGridSpec(
            num_scalar_prefetch=1,
            grid=(steps,),
            in_specs=[pl.BlockSpec((rows, n), lambda i, o: (i, 0))],
            out_specs=pl.BlockSpec((rows, n), lambda i, o: (o[0] + i, 0)),
        ),
        out_shape=jax.ShapeDtypeStruct((total_rows, n), v.dtype),
        cost_estimate=pl.CostEstimate(flops=10 * v.size, bytes_accessed=8 * v.size, transcendentals=0),
        name="place_first",
    )((block * steps).astype(jnp.int32)[None], v)


def head_kernel(
    n_glob, h_hbm, gamma_ref, beta_ref, b_ref, w_hbm, t_hbm,
    pb_hbm, pc_hbm, pd_hbm, du_ref, db_ref,
    h_s, acc_s, u_s, u_out, u_in, w_s, t_s, z_s, ra_s, b_s, db_s, g_s, ut_s, m_s, s_s, ts_s, tz_s, stat_s, col_s, du_s, du_in,
    h_sem, load_sem, u_sem, stat_send, stat_recv, sib_send, sib_recv, far_sem, du_sem, db_send, db_recv, out_sem, ready_sem,
):
    tokens, images, width = h_hbm.shape
    classes = w_hbm.shape[1]
    padded = w_s.shape[1]
    chunk = 512
    n_chunks = padded // chunk
    part = width // 8
    half = images // 2

    vp = lax.axis_index("vp")
    dp = lax.axis_index("dp")
    core, x, y = lax.rem(dp, 2), lax.rem(dp // 2, 2), dp // 4
    p1 = jnp.where(core == 0, x, y)
    p2 = jnp.where(core == 0, y, x)
    sib = dp + 1 - 2 * core
    along_x, along_y = dp + 2 - 4 * x, dp + 4 - 8 * y
    first = jnp.where(core == 0, along_x, along_y)
    z0 = lax.rem(vp, 2)
    near = vp + 1 - 2 * z0
    vp_size = stat_s.shape[0]
    others = [lax.rem(vp + k, vp_size) for k in range(1, vp_size)]

    barrier = pltpu.get_barrier_semaphore()
    for who in [(o, dp) for o in others] + [(vp, sib), (vp, along_x), (vp, along_y)]:
        pl.semaphore_signal(barrier, inc=1, device_id=who, device_id_type=MESH)

    quarter = images // 4
    block = h_s.shape[2]
    shared, blocks = quarter // block, 3 * quarter // block
    n_loads = 1
    while 2 * n_loads <= min(8, blocks):
        n_loads *= 2

    def first_row(i):
        return pl.multiple_of(jnp.where(i < shared, z0 * quarter + i * block, half + (i - shared) * block), block)

    def h_copy(i):
        slot = lax.rem(i, 2)
        return pltpu.make_async_copy(h_hbm.at[:, pl.ds(first_row(i), block), :], h_s.at[slot], h_sem.at[slot])

    def load(i):
        rows_w, rows_t = width // n_loads, images // n_loads
        at_w = pl.ds(pl.multiple_of(i * rows_w, rows_w), rows_w)
        at_t = pl.ds(pl.multiple_of(i * rows_t, rows_t), rows_t)
        cols = pl.ds(0, classes)
        pltpu.make_async_copy(w_hbm.at[at_w], w_s.at[at_w, cols], load_sem.at[0]).start()
        pltpu.make_async_copy(t_hbm.at[at_t], t_s.at[at_t, cols], load_sem.at[1]).start()

    h_copy(0).start()
    if padded > classes:
        b_s[:, classes:] = jnp.zeros((1, padded - classes), F32)
        w_s[:, classes:] = jnp.zeros((width, padded - classes), BF16)
        t_s[:, classes:] = jnp.zeros((t_s.shape[0], padded - classes), F32)
    b_s[:, :classes] = b_ref[...]
    m_s[...] = jnp.full_like(m_s, -jnp.inf)
    s_s[...] = jnp.zeros_like(s_s)
    ts_s[...] = jnp.zeros_like(ts_s)
    tz_s[...] = jnp.zeros_like(tz_s)
    limit = jnp.minimum(classes, NUM_CLASSES - vp * classes)

    def pool(i, carry):
        h_copy(i).wait()

        @pl.when(i + 1 < blocks)
        def _():
            h_copy(i + 1).start()

        @pl.when(i < n_loads)
        def _():
            load(i)

        slot = lax.rem(i, 2)
        acc_s[...] = jnp.zeros_like(acc_s)

        def group(j, carry):
            here = pl.ds(pl.multiple_of(j * 16, 16), 16)
            for t in range(tokens):
                c, r = norm_rows(h_s[slot, t, here, :].astype(F32))
                acc_s[here, :] += c * r
            return carry

        lax.fori_loop(0, block // 16, group, 0)
        u = acc_s[...] * (gamma_ref[...] * (1.0 / tokens)) + beta_ref[...]
        u_s[pl.ds(first_row(i), block), :] = u.astype(BF16)

        @pl.when(i < shared)
        def _():
            u_out[pl.ds(pl.multiple_of(i * block, block), block), :] = u

        return carry

    lax.fori_loop(0, shared, pool, 0)
    pl.semaphore_wait(barrier, vp_size + 2)
    u_copy = pltpu.make_async_remote_copy(
        src_ref=u_out, dst_ref=u_in, send_sem=u_sem.at[0], recv_sem=u_sem.at[1],
        device_id=(near, dp), device_id_type=MESH,
    )
    u_copy.start()
    lax.fori_loop(shared, blocks, pool, 0)
    u_copy.wait()
    u_s[pl.ds(pl.multiple_of((1 - z0) * quarter, quarter), quarter), :] = u_in[...].astype(BF16)
    pltpu.make_async_copy(w_hbm, w_s.at[:, pl.ds(0, classes)], load_sem.at[0]).wait()
    pltpu.make_async_copy(t_hbm, t_s.at[pl.ds(0, images), pl.ds(0, classes)], load_sem.at[1]).wait()

    def logits(i, carry):
        cols = pl.ds(pl.multiple_of(i * chunk, chunk), chunk)
        z = jnp.dot(u_s[...], w_s[:, cols], preferred_element_type=F32) + b_s[:, cols]
        valid = i * chunk + lax.broadcasted_iota(jnp.int32, (1, chunk), 1) < limit
        t = t_s[:images, cols]
        tz = t * jnp.where(valid, z, 0.0)
        z = jnp.where(valid, z, -jnp.inf)
        z_s[:images, cols] = z
        parts = [slice(k, k + 128) for k in range(0, chunk, 128)]
        m_old = m_s[...]
        m_new = m_old
        for p in parts:
            m_new = jnp.maximum(m_new, z[:, p])
        base = jnp.where(m_new == -jnp.inf, 0.0, m_new)
        s = s_s[...] * jnp.exp(m_old - base)
        ts = ts_s[...]
        tzs = tz_s[...]
        for p in parts:
            s += jnp.exp(z[:, p] - base)
            ts += t[:, p]
            tzs += tz[:, p]
        m_s[...] = m_new
        s_s[...] = s
        ts_s[...] = ts
        tz_s[...] = tzs
        return carry

    lax.fori_loop(0, n_chunks, logits, 0)

    m = m_s[...].max(axis=1, keepdims=True)
    s = (s_s[...] * jnp.exp(m_s[...] - m)).sum(axis=1, keepdims=True)
    ts = ts_s[...].sum(axis=1, keepdims=True)
    tz = tz_s[...].sum(axis=1, keepdims=True)
    lane = lax.broadcasted_iota(jnp.int32, m_s.shape, 1)
    packed = jnp.where(lane == 0, m, jnp.where(lane == 1, s, jnp.where(lane == 2, ts, tz)))
    stat_s[vp] = packed.T[:8]
    copies = []
    for k, o in enumerate(others):
        c = pltpu.make_async_remote_copy(
            src_ref=stat_s.at[vp], dst_ref=stat_s.at[vp], send_sem=stat_send.at[k], recv_sem=stat_recv.at[k],
            device_id=(o, dp), device_id_type=MESH,
        )
        c.start()
        copies.append(c)
    ut_s[...] = u_s[...].T
    for c in copies:
        c.wait()

    stat = [stat_s[k] for k in range(vp_size)]
    m = functools.reduce(jnp.maximum, [a[0:1] for a in stat])
    s = sum(a[1:2] * jnp.exp(a[0:1] - m) for a in stat)
    ts = sum(a[2:3] for a in stat)
    tz = sum(a[3:4] for a in stat)
    log_norm = m + jnp.log(s)
    loss = (log_norm * ts - tz).sum(axis=1, keepdims=True)
    row = lax.broadcasted_iota(jnp.int32, (128, m.shape[1]), 0)
    col_s[...] = jnp.where(row == 0, log_norm, ts).T

    def grads(i, carry):
        cols = pl.ds(pl.multiple_of(i * chunk, chunk), chunk)
        g = (jnp.exp(z_s[:images, cols] - col_s[:, 0:1]) * col_s[:, 1:2] - t_s[:images, cols]) * (1.0 / n_glob)
        g_s[:, cols] = g.astype(BF16)
        db_s[0, :, cols] = g.sum(axis=0, keepdims=True)
        return carry

    lax.fori_loop(0, n_chunks, grads, 0)
    db_s[0, :, classes:] = loss + jnp.zeros((1, padded - classes), F32)

    pl.semaphore_signal(ready_sem, inc=1, device_id=(vp, sib), device_id_type=MESH)

    def db_copy(k, who):
        return pltpu.make_async_remote_copy(
            src_ref=db_s.at[2 * k], dst_ref=db_s.at[2 * k + 1], send_sem=db_send.at[k], recv_sem=db_recv.at[k],
            device_id=(vp, who), device_id_type=MESH,
        )

    db_copies = [db_copy(0, sib), db_copy(1, along_x), db_copy(2, along_y)]

    def db_next(k):
        db_copies[k].wait()
        if k < 2:
            db_s[2 * k + 2] = db_s[2 * k] + db_s[2 * k + 1]
            db_copies[k + 1].start()
        else:
            db_ref[...] = db_s[4] + db_s[5]

    db_copies[0].start()

    mid = (n_chunks + 1) // 2
    split = mid * chunk

    def dots(src, n, dst, add, lo=0, hi=n_chunks):
        left = ut_s[pl.ds(pl.multiple_of(src * part, part), n), :]

        def body(i, carry):
            cols = pl.ds(pl.multiple_of(i * chunk, chunk), chunk)
            v = jnp.dot(left, g_s[:, cols], preferred_element_type=F32)
            at = pl.ds(dst, n)
            if add:
                t_s[at, cols] = t_s[at, cols] + v
            else:
                z_s[at, cols] = v
            return carry

        lax.fori_loop(lo, hi, body, 0)

    def to_sibling(k, at, n, lo=0, hi=classes):
        rows = pl.ds(pl.multiple_of(at * part, part), part)
        cols = pl.ds(lo, hi - lo)
        return pltpu.make_async_remote_copy(
            src_ref=z_s.at[rows, cols], dst_ref=t_s.at[pl.ds(k * part, part), cols],
            send_sem=sib_send.at[n], recv_sem=sib_recv.at[n], device_id=(vp, sib), device_id_type=MESH,
        )

    def to_first(n, lo, hi):
        cols = pl.ds(lo, hi - lo)
        return pltpu.make_async_remote_copy(
            src_ref=t_s.at[pl.ds(0, part), cols], dst_ref=ra_s.at[:, cols],
            send_sem=far_sem.at[0, n], recv_sem=far_sem.at[1, n], device_id=(vp, first), device_id_type=MESH,
        )

    halves = ((0, mid, 0, split), (mid, n_chunks, split, classes))
    pair = 4 * (1 - core) + 2 * (1 - p2)
    sends = [to_sibling(0, 0, n, lo, hi) for n, (_, _, lo, hi) in enumerate(halves)]
    sends += [to_sibling(1, 1, 2), to_sibling(2, 3 - p1, 3), to_sibling(3, 2 + p1, 4)]
    dots(pair + 1 - p1, part, 0, False, *halves[0][:2])
    pl.semaphore_wait(ready_sem, 1)
    sends[0].start()
    dots(pair + 1 - p1, part, 0, False, *halves[1][:2])
    sends[1].start()
    db_next(0)
    dots(pair + p1, part, part, False)
    sends[2].start()
    db_next(1)
    own = [4 * core + 2 * a + b for a, b in ((1 - p1, 1 - p2), (1 - p1, p2), (p1, 1 - p2), (p1, p2))]
    far = []
    for n, (i0, i1, lo, hi) in enumerate(halves):
        sends[n].wait_recv()
        dots(own[0], part, 0, True, i0, i1)
        c = to_first(n, lo, hi)
        c.start()
        far.append(c)
    dots(4 * (1 - core) + 2 * p2, 2 * part, 2 * part, False)
    sends[3].start()
    sends[4].start()

    def piece(k):
        return t_s.at[pl.ds(k * part, part), pl.ds(0, classes)]

    def du_dot(i, carry):
        cols = pl.ds(pl.multiple_of(i * chunk, chunk), chunk)
        v = lax.dot_general(g_s[:, cols], w_s[:, cols], (((1,), (1,)), ((), ())), preferred_element_type=F32)
        du_s[...] = du_s[...] + v
        return carry

    du_s[...] = jnp.zeros_like(du_s)
    lax.fori_loop(0, n_chunks, du_dot, 0)
    keep = pl.ds(pl.multiple_of(z0 * half, half), half)
    give = pl.ds(pl.multiple_of((1 - z0) * half, half), half)
    du_copy = pltpu.make_async_remote_copy(
        src_ref=du_s.at[give], dst_ref=du_in, send_sem=du_sem.at[0], recv_sem=du_sem.at[1],
        device_id=(near, dp), device_id_type=MESH,
    )
    du_copy.start()
    db_next(2)

    outs = []
    for k, out in ((1, pb_hbm), (2, pc_hbm), (3, pd_hbm)):
        sends[k + 1].wait_recv()
        dots(own[k], part, k * part, True)
        c = pltpu.make_async_copy(piece(k), out, out_sem.at[k - 1])
        if k != 2:
            c.start()
        outs.append(c)
    for c in sends:
        c.wait_send()
    du_copy.wait()
    du_ref[...] = du_s[keep, :] + du_in[...]
    for c in far:
        c.wait()

    def add_far(i, carry):
        cols = pl.ds(pl.multiple_of(i * 128, 128), 128)
        at = pl.ds(2 * part, part)
        t_s[at, cols] = t_s[at, cols] + ra_s[:, cols]
        return carry

    lax.fori_loop(0, classes // 128, add_far, 0)
    outs[1].start()
    for c in outs:
        c.wait()


def head(ht, gamma, beta, b, w, t, n_glob, vp_size):
    tokens, images, width = ht.shape
    classes = w.shape[1]
    padded = (classes // 512 + 1) * 512
    part = width // 8
    rows = max(images, 4 * part)
    quarter = images // 4
    block = min(32, quarter)
    any_spec = pl.BlockSpec(memory_space=pl.ANY)
    vmem = pl.BlockSpec(memory_space=pltpu.VMEM)
    dma = pltpu.SemaphoreType.DMA
    piece = jax.ShapeDtypeStruct((part, classes), F32)
    return pl.pallas_call(
        functools.partial(head_kernel, n_glob),
        in_specs=[any_spec, vmem, vmem, vmem, any_spec, any_spec],
        out_specs=[any_spec] * 3 + [vmem] * 2,
        out_shape=[piece] * 3 + [
            jax.ShapeDtypeStruct((images // 2, width), F32),
            jax.ShapeDtypeStruct((1, padded), F32),
        ],
        scratch_shapes=[
            pltpu.VMEM((2, tokens, block, width), BF16),
            pltpu.VMEM((block, width), F32),
            pltpu.VMEM((images, width), BF16),
            pltpu.VMEM((quarter, width), F32),
            pltpu.VMEM((quarter, width), F32),
            pltpu.VMEM((width, padded), BF16),
            pltpu.VMEM((rows, padded), F32),
            pltpu.VMEM((rows, padded), F32),
            pltpu.VMEM((part, classes), F32),
            pltpu.VMEM((1, padded), F32),
            pltpu.VMEM((6, 1, padded), F32),
            pltpu.VMEM((images, padded), BF16),
            pltpu.VMEM((width, images), BF16),
        ] + [pltpu.VMEM((images, 128), F32)] * 4 + [
            pltpu.VMEM((vp_size, 8, images), F32),
            pltpu.VMEM((images, 128), F32),
            pltpu.VMEM((images, width), F32),
            pltpu.VMEM((images // 2, width), F32),
            dma((2,)),
            dma((2,)),
            dma((2,)),
            dma((vp_size - 1,)),
            dma((vp_size - 1,)),
            dma((5,)),
            dma((5,)),
            dma((2, 2)),
            dma((2,)),
            dma((3,)),
            dma((3,)),
            dma((3,)),
            pltpu.SemaphoreType.REGULAR,
        ],
        compiler_params=pltpu.CompilerParams(
            collective_id=0, has_side_effects=True, vmem_limit_bytes=60 * 1024 * 1024
        ),
        cost_estimate=pl.CostEstimate(
            flops=6 * images * width * classes, bytes_accessed=20 * width * classes, transcendentals=0
        ),
        name="head",
    )(ht, gamma[None], beta[None], b[None], w, t)


def solution(mesh):
    dp_size = mesh.shape["dp"]
    vp_size = mesh.shape["vp"]
    sibling = [(i, i ^ 1) for i in range(8)]
    first = [(i, i ^ (4 if i & 1 else 2)) for i in range(8)]
    second = [(i, i ^ (2 if i & 1 else 4)) for i in range(8)]
    near = [(i, i ^ 1) for i in range(vp_size)]
    distant = [(i, i ^ 2) for i in range(vp_size)]

    def local_step(h_loc, gamma, beta, w_loc, b_loc, t_loc):
        images, _, width = h_loc.shape
        n_glob = images * dp_size
        classes = w_loc.shape[1]
        part = width // 8
        quarter = images // 4
        dp = lax.axis_index("dp")
        vp = lax.axis_index("vp")
        core, x, y = dp & 1, (dp >> 1) & 1, dp >> 2
        z0, z1 = vp & 1, vp >> 1
        p1 = jnp.where(core == 0, x, y)
        p2 = jnp.where(core == 0, y, x)
        own = [4 * core + 2 * a + b for a, b in ((1 - p1, 1 - p2), (1 - p1, p2), (p1, 1 - p2), (p1, p2))]
        sib = [4 * (1 - core) + 2 * a + b for a, b in ((1 - p2, 1 - p1), (1 - p2, p1), (p2, 1 - p1), (p2, p1))]

        ht = h_loc.transpose(1, 0, 2)
        b, c, d, du_half, db = head(ht, gamma, beta, b_loc, w_loc, t_loc, n_glob, vp_size)

        def send(v, pairs):
            return lax.ppermute(v, "dp", pairs)

        r_d = send(b, first)
        r_d2 = send(c, second)

        got = lax.ppermute(lax.dynamic_slice(du_half, ((1 - z1) * quarter, 0), (quarter, width)), "vp", distant)
        du_own = lax.dynamic_slice(du_half, (z1 * quarter, 0), (quarter, width)) + got
        du_far = lax.ppermute(du_own, "vp", distant)
        du_near = lax.ppermute(du_own, "vp", near)
        du_last = lax.ppermute(du_far, "vp", near)

        dh, token = pool_backward(ht, du_own, gamma, None, 2 * z0 + z1, du_own)
        d = ((d + r_d) + r_d2) + token[0, 0]
        c_fin = send(d, second)
        b_fin = send(d, first)
        dh, token = pool_backward(ht, du_far, gamma, dh, 2 * z0 + 1 - z1, d)
        dh, token = pool_backward(ht, du_near, gamma, dh, 2 * (1 - z0) + z1, token)
        dh, token = pool_backward(ht, du_last, gamma, dh, 2 * (1 - z0) + 1 - z1, token)
        a_fin = send(c_fin, first)
        mine = [a_fin, b_fin, c_fin, d]
        theirs = [send(v, sibling) for v in mine]

        out = place_first(d, own[3], width)
        for v, k in ((theirs[3], sib[3]), (mine[2], own[2]), (theirs[2], sib[2]),
                     (mine[1], own[1]), (theirs[1], sib[1]), (mine[0], own[0]), (theirs[0], sib[0])):
            out = lax.dynamic_update_slice(out, v, (k * part, 0))
        loss, db = db[0, classes] / n_glob, db[0, :classes]
        return loss, out, db, dh.transpose(1, 0, 2)

    return jax.shard_map(
        local_step,
        mesh=mesh,
        in_specs=(P("dp", None, None), P(), P(), P(None, "vp"), P("vp"), P("dp", "vp")),
        out_specs=(P(), P(None, "vp"), P("vp"), P("dp", None, None)),
        check_vma=False,
    )
```

```python
import functools

import jax
import jax.numpy as jnp
from jax import lax
from jax.experimental import pallas as pl
from jax.experimental.pallas import tpu as pltpu
from jax.sharding import PartitionSpec as P


NUM_CLASSES = 21841
LN_EPS = 1e-5
F32 = jnp.float32
BF16 = jnp.bfloat16
MESH = pl.DeviceIdType.MESH


def norm_rows(x):
    width = x.shape[-1]
    c = x - x.sum(axis=-1, keepdims=True) * (1.0 / width)
    var = (c * c).sum(axis=-1, keepdims=True) * (1.0 / width)
    return c, lax.rsqrt(var + LN_EPS)


def pool_backward_kernel(off_ref, h_ref, du_ref, gamma_ref, *rest):
    dh_ref, token_ref, v_ref = rest[-3:]
    tokens, rows, width = h_ref.shape
    v = du_ref[...] * (gamma_ref[...] * (1.0 / tokens))
    v_ref[...] = v - v.sum(axis=-1, keepdims=True) * (1.0 / width)
    token_ref[...] = jnp.zeros_like(token_ref)

    def group(i, carry):
        here = pl.ds(pl.multiple_of(i * 16, 16), 16)
        for t in range(tokens):
            c, r = norm_rows(h_ref[t, here, :].astype(F32))
            vc = v_ref[here, :]
            xhat = c * r
            k = (vc * xhat).sum(axis=-1, keepdims=True) * (1.0 / width)
            dh_ref[t, here, :] = ((vc - xhat * k) * r).astype(BF16)
        return carry

    lax.fori_loop(0, rows // 16, group, 0)


def pool_backward(ht, du, gamma, buf, block, after, rows=32):
    tokens, images, width = ht.shape
    count = du.shape[0]
    rows = min(rows, count)
    steps = count // rows
    any_spec = pl.BlockSpec(memory_space=pl.ANY)
    in_specs = [
        pl.BlockSpec((tokens, rows, width), lambda i, o: (0, o[0] + i, 0)),
        pl.BlockSpec((rows, width), lambda i, o: (i, 0)),
        pl.BlockSpec((1, width), lambda i, o: (0, 0)),
        any_spec,
    ]
    args = [(block * steps).astype(jnp.int32)[None], ht, du, gamma[None], after]
    aliases = {}
    if buf is not None:
        in_specs.append(any_spec)
        args.append(buf)
        aliases = {5: 0}
    return pl.pallas_call(
        pool_backward_kernel,
        grid_spec=pltpu.PrefetchScalarGridSpec(
            num_scalar_prefetch=1,
            grid=(steps,),
            in_specs=in_specs,
            out_specs=[
                pl.BlockSpec((tokens, rows, width), lambda i, o: (0, o[0] + i, 0)),
                pl.BlockSpec((8, 128), lambda i, o: (0, 0)),
            ],
            scratch_shapes=[pltpu.VMEM((rows, width), F32)],
        ),
        out_shape=[
            jax.ShapeDtypeStruct((tokens, images, width), BF16),
            jax.ShapeDtypeStruct((8, 128), F32),
        ],
        input_output_aliases=aliases,
        compiler_params=pltpu.CompilerParams(dimension_semantics=("arbitrary",)),
        cost_estimate=pl.CostEstimate(
            flops=40 * 12 * tokens * count * width, bytes_accessed=4 * tokens * count * width, transcendentals=0
        ),
        name="pool_backward",
    )(*args)


def place_kernel(off_ref, v_ref, o_ref):
    o_ref[...] = v_ref[...]


def place_first(v, block, total_rows, rows=32):
    count, n = v.shape
    steps = count // rows
    return pl.pallas_call(
        place_kernel,
        grid_spec=pltpu.PrefetchScalarGridSpec(
            num_scalar_prefetch=1,
            grid=(steps,),
            in_specs=[pl.BlockSpec((rows, n), lambda i, o: (i, 0))],
            out_specs=pl.BlockSpec((rows, n), lambda i, o: (o[0] + i, 0)),
        ),
        out_shape=jax.ShapeDtypeStruct((total_rows, n), v.dtype),
        cost_estimate=pl.CostEstimate(flops=10 * v.size, bytes_accessed=8 * v.size, transcendentals=0),
        name="place_first",
    )((block * steps).astype(jnp.int32)[None], v)


def head_kernel(
    n_glob, h_hbm, gamma_ref, beta_ref, b_ref, w_hbm, t_hbm,
    pb_hbm, pc_hbm, pd_hbm, du_ref, db_ref,
    h_s, acc_s, u_s, u_out, u_in, w_s, t_s, z_s, ra_s, b_s, db_s, g_s, ut_s, m_s, s_s, ts_s, tz_s, stat_s, col_s, du_s, du_in,
    h_sem, load_sem, u_sem, stat_send, stat_recv, sib_send, sib_recv, far_sem, du_sem, db_send, db_recv, out_sem, ready_sem,
):
    tokens, images, width = h_hbm.shape
    classes = w_hbm.shape[1]
    padded = w_s.shape[1]
    chunk = 512
    n_chunks = padded // chunk
    part = width // 8
    half = images // 2

    vp = lax.axis_index("vp")
    dp = lax.axis_index("dp")
    core, x, y = lax.rem(dp, 2), lax.rem(dp // 2, 2), dp // 4
    p1 = jnp.where(core == 0, x, y)
    p2 = jnp.where(core == 0, y, x)
    sib = dp + 1 - 2 * core
    along_x, along_y = dp + 2 - 4 * x, dp + 4 - 8 * y
    first = jnp.where(core == 0, along_x, along_y)
    z0 = lax.rem(vp, 2)
    near = vp + 1 - 2 * z0
    vp_size = stat_s.shape[0]
    others = [lax.rem(vp + k, vp_size) for k in range(1, vp_size)]

    barrier = pltpu.get_barrier_semaphore()
    for who in [(o, dp) for o in others] + [(vp, sib), (vp, along_x), (vp, along_y)]:
        pl.semaphore_signal(barrier, inc=1, device_id=who, device_id_type=MESH)

    quarter = images // 4
    block = h_s.shape[2]
    shared, blocks = quarter // block, 3 * quarter // block
    n_loads = 1
    while 2 * n_loads <= min(8, blocks):
        n_loads *= 2

    def first_row(i):
        return pl.multiple_of(jnp.where(i < shared, z0 * quarter + i * block, half + (i - shared) * block), block)

    def h_copy(i):
        slot = lax.rem(i, 2)
        return pltpu.make_async_copy(h_hbm.at[:, pl.ds(first_row(i), block), :], h_s.at[slot], h_sem.at[slot])

    def load(i):
        rows_w, rows_t = width // n_loads, images // n_loads
        at_w = pl.ds(pl.multiple_of(i * rows_w, rows_w), rows_w)
        at_t = pl.ds(pl.multiple_of(i * rows_t, rows_t), rows_t)
        cols = pl.ds(0, classes)
        pltpu.make_async_copy(w_hbm.at[at_w], w_s.at[at_w, cols], load_sem.at[0]).start()
        pltpu.make_async_copy(t_hbm.at[at_t], t_s.at[at_t, cols], load_sem.at[1]).start()

    h_copy(0).start()
    if padded > classes:
        b_s[:, classes:] = jnp.zeros((1, padded - classes), F32)
        w_s[:, classes:] = jnp.zeros((width, padded - classes), BF16)
        t_s[:, classes:] = jnp.zeros((t_s.shape[0], padded - classes), F32)
    b_s[:, :classes] = b_ref[...]
    m_s[...] = jnp.full_like(m_s, -jnp.inf)
    s_s[...] = jnp.zeros_like(s_s)
    ts_s[...] = jnp.zeros_like(ts_s)
    tz_s[...] = jnp.zeros_like(tz_s)
    limit = jnp.minimum(classes, NUM_CLASSES - vp * classes)

    def pool(i, carry):
        h_copy(i).wait()

        @pl.when(i + 1 < blocks)
        def _():
            h_copy(i + 1).start()

        @pl.when(i < n_loads)
        def _():
            load(i)

        slot = lax.rem(i, 2)
        acc_s[...] = jnp.zeros_like(acc_s)

        def group(j, carry):
            here = pl.ds(pl.multiple_of(j * 16, 16), 16)
            for t in range(tokens):
                c, r = norm_rows(h_s[slot, t, here, :].astype(F32))
                acc_s[here, :] += c * r
            return carry

        lax.fori_loop(0, block // 16, group, 0)
        u = acc_s[...] * (gamma_ref[...] * (1.0 / tokens)) + beta_ref[...]
        u_s[pl.ds(first_row(i), block), :] = u.astype(BF16)

        @pl.when(i < shared)
        def _():
            u_out[pl.ds(pl.multiple_of(i * block, block), block), :] = u

        return carry

    lax.fori_loop(0, shared, pool, 0)
    pl.semaphore_wait(barrier, vp_size + 2)
    u_copy = pltpu.make_async_remote_copy(
        src_ref=u_out, dst_ref=u_in, send_sem=u_sem.at[0], recv_sem=u_sem.at[1],
        device_id=(near, dp), device_id_type=MESH,
    )
    u_copy.start()
    lax.fori_loop(shared, blocks, pool, 0)
    u_copy.wait()
    u_s[pl.ds(pl.multiple_of((1 - z0) * quarter, quarter), quarter), :] = u_in[...].astype(BF16)
    pltpu.make_async_copy(w_hbm, w_s.at[:, pl.ds(0, classes)], load_sem.at[0]).wait()
    pltpu.make_async_copy(t_hbm, t_s.at[pl.ds(0, images), pl.ds(0, classes)], load_sem.at[1]).wait()

    def logits(i, carry):
        cols = pl.ds(pl.multiple_of(i * chunk, chunk), chunk)
        z = jnp.dot(u_s[...], w_s[:, cols], preferred_element_type=F32) + b_s[:, cols]
        valid = i * chunk + lax.broadcasted_iota(jnp.int32, (1, chunk), 1) < limit
        t = t_s[:images, cols]
        tz = t * jnp.where(valid, z, 0.0)
        z = jnp.where(valid, z, -jnp.inf)
        z_s[:images, cols] = z
        parts = [slice(k, k + 128) for k in range(0, chunk, 128)]
        m_old = m_s[...]
        m_new = m_old
        for p in parts:
            m_new = jnp.maximum(m_new, z[:, p])
        base = jnp.where(m_new == -jnp.inf, 0.0, m_new)
        s = s_s[...] * jnp.exp(m_old - base)
        ts = ts_s[...]
        tzs = tz_s[...]
        for p in parts:
            s += jnp.exp(z[:, p] - base)
            ts += t[:, p]
            tzs += tz[:, p]
        m_s[...] = m_new
        s_s[...] = s
        ts_s[...] = ts
        tz_s[...] = tzs
        return carry

    lax.fori_loop(0, n_chunks, logits, 0)

    m = m_s[...].max(axis=1, keepdims=True)
    s = (s_s[...] * jnp.exp(m_s[...] - m)).sum(axis=1, keepdims=True)
    ts = ts_s[...].sum(axis=1, keepdims=True)
    tz = tz_s[...].sum(axis=1, keepdims=True)
    lane = lax.broadcasted_iota(jnp.int32, m_s.shape, 1)
    packed = jnp.where(lane == 0, m, jnp.where(lane == 1, s, jnp.where(lane == 2, ts, tz)))
    stat_s[vp] = packed.T[:8]
    copies = []
    for k, o in enumerate(others):
        c = pltpu.make_async_remote_copy(
            src_ref=stat_s.at[vp], dst_ref=stat_s.at[vp], send_sem=stat_send.at[k], recv_sem=stat_recv.at[k],
            device_id=(o, dp), device_id_type=MESH,
        )
        c.start()
        copies.append(c)
    ut_s[...] = u_s[...].T
    for c in copies:
        c.wait()

    stat = [stat_s[k] for k in range(vp_size)]
    m = functools.reduce(jnp.maximum, [a[0:1] for a in stat])
    s = sum(a[1:2] * jnp.exp(a[0:1] - m) for a in stat)
    ts = sum(a[2:3] for a in stat)
    tz = sum(a[3:4] for a in stat)
    log_norm = m + jnp.log(s)
    loss = (log_norm * ts - tz).sum(axis=1, keepdims=True)
    row = lax.broadcasted_iota(jnp.int32, (128, m.shape[1]), 0)
    col_s[...] = jnp.where(row == 0, log_norm, ts).T

    def grads(i, carry):
        cols = pl.ds(pl.multiple_of(i * chunk, chunk), chunk)
        g = (jnp.exp(z_s[:images, cols] - col_s[:, 0:1]) * col_s[:, 1:2] - t_s[:images, cols]) * (1.0 / n_glob)
        g_s[:, cols] = g.astype(BF16)
        db_s[0, :, cols] = g.sum(axis=0, keepdims=True)
        return carry

    lax.fori_loop(0, n_chunks, grads, 0)
    db_s[0, :, classes:] = loss + jnp.zeros((1, padded - classes), F32)

    pl.semaphore_signal(ready_sem, inc=1, device_id=(vp, sib), device_id_type=MESH)

    def db_copy(k, who):
        return pltpu.make_async_remote_copy(
            src_ref=db_s.at[2 * k], dst_ref=db_s.at[2 * k + 1], send_sem=db_send.at[k], recv_sem=db_recv.at[k],
            device_id=(vp, who), device_id_type=MESH,
        )

    db_copies = [db_copy(0, sib), db_copy(1, along_x), db_copy(2, along_y)]

    def db_next(k):
        db_copies[k].wait()
        if k < 2:
            db_s[2 * k + 2] = db_s[2 * k] + db_s[2 * k + 1]
            db_copies[k + 1].start()
        else:
            db_ref[...] = db_s[4] + db_s[5]

    db_copies[0].start()

    mid = (n_chunks + 1) // 2
    split = mid * chunk

    def dots(src, n, dst, add, lo=0, hi=n_chunks):
        left = ut_s[pl.ds(pl.multiple_of(src * part, part), n), :]

        def body(i, carry):
            cols = pl.ds(i * chunk if isinstance(i, int) else pl.multiple_of(i * chunk, chunk), chunk)
            v = jnp.dot(left, g_s[:, cols], preferred_element_type=F32)
            at = pl.ds(dst, n)
            if add:
                t_s[at, cols] = t_s[at, cols] + v
            else:
                z_s[at, cols] = v
            return carry

        if n == part and hi - lo < n_chunks:
            for i in range(lo, hi):
                body(i, 0)
        else:
            lax.fori_loop(lo, hi, body, 0)

    def to_sibling(k, at, n, lo=0, hi=classes):
        rows = pl.ds(pl.multiple_of(at * part, part), part)
        cols = pl.ds(lo, hi - lo)
        return pltpu.make_async_remote_copy(
            src_ref=z_s.at[rows, cols], dst_ref=t_s.at[pl.ds(k * part, part), cols],
            send_sem=sib_send.at[n], recv_sem=sib_recv.at[n], device_id=(vp, sib), device_id_type=MESH,
        )

    def to_first(n, lo, hi):
        cols = pl.ds(lo, hi - lo)
        return pltpu.make_async_remote_copy(
            src_ref=t_s.at[pl.ds(0, part), cols], dst_ref=ra_s.at[:, cols],
            send_sem=far_sem.at[0, n], recv_sem=far_sem.at[1, n], device_id=(vp, first), device_id_type=MESH,
        )

    halves = ((0, mid, 0, split), (mid, n_chunks, split, classes))
    pair = 4 * (1 - core) + 2 * (1 - p2)
    sends = [to_sibling(0, 0, n, lo, hi) for n, (_, _, lo, hi) in enumerate(halves)]
    sends += [to_sibling(1, 1, 2), to_sibling(2, 3 - p1, 3), to_sibling(3, 2 + p1, 4)]
    dots(pair + 1 - p1, part, 0, False, *halves[0][:2])
    pl.semaphore_wait(ready_sem, 1)
    sends[0].start()
    dots(pair + 1 - p1, part, 0, False, *halves[1][:2])
    sends[1].start()
    db_next(0)
    dots(pair + p1, part, part, False)
    sends[2].start()
    db_next(1)
    own = [4 * core + 2 * a + b for a, b in ((1 - p1, 1 - p2), (1 - p1, p2), (p1, 1 - p2), (p1, p2))]
    far = []
    for n, (i0, i1, lo, hi) in enumerate(halves):
        sends[n].wait_recv()
        dots(own[0], part, 0, True, i0, i1)
        c = to_first(n, lo, hi)
        c.start()
        far.append(c)

    def piece(k):
        return t_s.at[pl.ds(k * part, part), pl.ds(0, classes)]

    def du_dots(at):
        def body(i, carry):
            cols = pl.ds(pl.multiple_of(i * chunk, chunk), chunk)
            v = lax.dot_general(g_s[at, cols], w_s[:, cols], (((1,), (1,)), ((), ())), preferred_element_type=F32)
            du_s[at, :] = du_s[at, :] + v
            return carry

        lax.fori_loop(0, n_chunks, body, 0)

    du_s[...] = jnp.zeros_like(du_s)
    keep = pl.ds(pl.multiple_of(z0 * half, half), half)
    give = pl.ds(pl.multiple_of((1 - z0) * half, half), half)
    du_dots(give)
    du_copy = pltpu.make_async_remote_copy(
        src_ref=du_s.at[give], dst_ref=du_in, send_sem=du_sem.at[0], recv_sem=du_sem.at[1],
        device_id=(near, dp), device_id_type=MESH,
    )
    du_copy.start()
    dots(4 * (1 - core) + 2 * p2, 2 * part, 2 * part, False)
    sends[3].start()
    sends[4].start()
    db_next(2)
    du_dots(keep)

    outs = []
    for k, out in ((1, pb_hbm), (2, None), (3, pd_hbm)):
        sends[k + 1].wait_recv()
        dots(own[k], part, k * part, True)
        if out is not None:
            c = pltpu.make_async_copy(piece(k), out, out_sem.at[k - 1])
            c.start()
            outs.append(c)
    for c in sends:
        c.wait_send()
    du_copy.wait()
    du_ref[...] = du_s[keep, :] + du_in[...]
    for n, (_, _, lo, hi) in enumerate(halves):
        far[n].wait()

        def add_far(i, carry):
            cols = pl.ds(pl.multiple_of(i * 128, 128), 128)
            at = pl.ds(2 * part, part)
            t_s[at, cols] = t_s[at, cols] + ra_s[:, cols]
            return carry

        lax.fori_loop(lo // 128, hi // 128, add_far, 0)
        cols = pl.ds(lo, hi - lo)
        c = pltpu.make_async_copy(t_s.at[pl.ds(2 * part, part), cols], pc_hbm.at[:, cols], out_sem.at[1 + 2 * n])
        c.start()
        outs.append(c)
    for c in outs:
        c.wait()


def head(ht, gamma, beta, b, w, t, n_glob, vp_size):
    tokens, images, width = ht.shape
    classes = w.shape[1]
    padded = (classes // 512 + 1) * 512
    part = width // 8
    rows = max(images, 4 * part)
    quarter = images // 4
    block = min(32, quarter)
    any_spec = pl.BlockSpec(memory_space=pl.ANY)
    vmem = pl.BlockSpec(memory_space=pltpu.VMEM)
    dma = pltpu.SemaphoreType.DMA
    piece = jax.ShapeDtypeStruct((part, classes), F32)
    return pl.pallas_call(
        functools.partial(head_kernel, n_glob),
        in_specs=[any_spec, vmem, vmem, vmem, any_spec, any_spec],
        out_specs=[any_spec] * 3 + [vmem] * 2,
        out_shape=[piece] * 3 + [
            jax.ShapeDtypeStruct((images // 2, width), F32),
            jax.ShapeDtypeStruct((1, padded), F32),
        ],
        scratch_shapes=[
            pltpu.VMEM((2, tokens, block, width), BF16),
            pltpu.VMEM((block, width), F32),
            pltpu.VMEM((images, width), BF16),
            pltpu.VMEM((quarter, width), F32),
            pltpu.VMEM((quarter, width), F32),
            pltpu.VMEM((width, padded), BF16),
            pltpu.VMEM((rows, padded), F32),
            pltpu.VMEM((rows, padded), F32),
            pltpu.VMEM((part, classes), F32),
            pltpu.VMEM((1, padded), F32),
            pltpu.VMEM((6, 1, padded), F32),
            pltpu.VMEM((images, padded), BF16),
            pltpu.VMEM((width, images), BF16),
        ] + [pltpu.VMEM((images, 128), F32)] * 4 + [
            pltpu.VMEM((vp_size, 8, images), F32),
            pltpu.VMEM((images, 128), F32),
            pltpu.VMEM((images, width), F32),
            pltpu.VMEM((images // 2, width), F32),
            dma((2,)),
            dma((2,)),
            dma((2,)),
            dma((vp_size - 1,)),
            dma((vp_size - 1,)),
            dma((5,)),
            dma((5,)),
            dma((2, 2)),
            dma((2,)),
            dma((3,)),
            dma((3,)),
            dma((4,)),
            pltpu.SemaphoreType.REGULAR,
        ],
        compiler_params=pltpu.CompilerParams(
            collective_id=0, has_side_effects=True, vmem_limit_bytes=60 * 1024 * 1024
        ),
        cost_estimate=pl.CostEstimate(
            flops=6 * images * width * classes, bytes_accessed=20 * width * classes, transcendentals=0
        ),
        name="head",
    )(ht, gamma[None], beta[None], b[None], w, t)


def solution(mesh):
    dp_size = mesh.shape["dp"]
    vp_size = mesh.shape["vp"]
    sibling = [(i, i ^ 1) for i in range(8)]
    first = [(i, i ^ (4 if i & 1 else 2)) for i in range(8)]
    second = [(i, i ^ (2 if i & 1 else 4)) for i in range(8)]
    near = [(i, i ^ 1) for i in range(vp_size)]
    distant = [(i, i ^ 2) for i in range(vp_size)]

    def local_step(h_loc, gamma, beta, w_loc, b_loc, t_loc):
        images, _, width = h_loc.shape
        n_glob = images * dp_size
        classes = w_loc.shape[1]
        part = width // 8
        quarter = images // 4
        dp = lax.axis_index("dp")
        vp = lax.axis_index("vp")
        core, x, y = dp & 1, (dp >> 1) & 1, dp >> 2
        z0, z1 = vp & 1, vp >> 1
        p1 = jnp.where(core == 0, x, y)
        p2 = jnp.where(core == 0, y, x)
        own = [4 * core + 2 * a + b for a, b in ((1 - p1, 1 - p2), (1 - p1, p2), (p1, 1 - p2), (p1, p2))]
        sib = [4 * (1 - core) + 2 * a + b for a, b in ((1 - p2, 1 - p1), (1 - p2, p1), (p2, 1 - p1), (p2, p1))]

        ht = h_loc.transpose(1, 0, 2)
        b, c, d, du_half, db = head(ht, gamma, beta, b_loc, w_loc, t_loc, n_glob, vp_size)

        def send(v, pairs):
            return lax.ppermute(v, "dp", pairs)

        r_d = send(b, first)
        r_d2 = send(c, second)

        got = lax.ppermute(lax.dynamic_slice(du_half, ((1 - z1) * quarter, 0), (quarter, width)), "vp", distant)
        du_own = lax.dynamic_slice(du_half, (z1 * quarter, 0), (quarter, width)) + got
        du_far = lax.ppermute(du_own, "vp", distant)
        du_near = lax.ppermute(du_own, "vp", near)
        du_last = lax.ppermute(du_far, "vp", near)

        dh, token = pool_backward(ht, du_own, gamma, None, 2 * z0 + z1, du_own)
        d = ((d + r_d) + r_d2) + token[0, 0]
        c_fin = send(d, second)
        b_fin = send(d, first)
        dh, token = pool_backward(ht, du_far, gamma, dh, 2 * z0 + 1 - z1, d)
        dh, token = pool_backward(ht, du_near, gamma, dh, 2 * (1 - z0) + z1, token)
        dh, token = pool_backward(ht, du_last, gamma, dh, 2 * (1 - z0) + 1 - z1, token)
        a_fin = []
        for k in range(2):
            a_fin.append(send(c_fin[k * part // 2 : (k + 1) * part // 2], first))
        mine = a_fin + [b_fin, c_fin, d]
        theirs = [send(v, sibling) for v in mine]

        out = place_first(d, own[3], width)
        places = [(theirs[4], sib[3], 0), (mine[3], own[2], 0), (theirs[3], sib[2], 0), (mine[2], own[1], 0),
                  (theirs[2], sib[1], 0), (mine[0], own[0], 0), (theirs[0], sib[0], 0),
                  (mine[1], own[0], part // 2), (theirs[1], sib[0], part // 2)]
        for v, k, off in places:
            out = lax.dynamic_update_slice(out, v, (k * part + off, 0))
        loss, db = db[0, classes] / n_glob, db[0, :classes]
        return loss, out, db, dh.transpose(1, 0, 2)

    return jax.shard_map(
        local_step,
        mesh=mesh,
        in_specs=(P("dp", None, None), P(), P(), P(None, "vp"), P("vp"), P("dp", "vp")),
        out_specs=(P(), P(None, "vp"), P("vp"), P("dp", None, None)),
        check_vma=False,
    )
```
